32 devices in a mesh: pp: 2 (over core), ep: 16 (over z, y, x), tp: 1.
Axes of the slice: x: 2, y: 2, z: 4, core: 2. Of those that a mesh axis runs over, the one named last changes fastest.
Arguments:
- acts: bfloat16 [2, 96, 3072], P(None, 'ep'), may hold values from -6 to 6
- route_ids: int32 [2, 2, 96, 8], P('pp', None, 'ep'), may hold values from 0 to 23, all different within a row; in each aligned block of 6 rows (0 to 5, 6 to 11, ..., all dimensions but the last counted through in order) at most 2 rows name the same one
- norm_gain: bfloat16 [2, 3072], P('pp'), may hold values from 0.5 to 1.5
- router: bfloat16 [2, 3072, 24], P('pp'), may hold values from -0.109375 to 0.109375
- dense_gate: bfloat16 [2, 3072, 6144], P('pp', None, ('ep', 'tp')), may hold values from -0.109375 to 0.109375
- dense_up: bfloat16 [2, 3072, 6144], P('pp', None, ('ep', 'tp')), may hold values from -0.109375 to 0.109375
- dense_down: bfloat16 [2, 6144, 3072], P('pp', ('ep', 'tp')), may hold values from -0.078125 to 0.078125
- expert_gate: bfloat16 [2, 16, 3072, 1024], P('pp', 'ep', None, 'tp'), may hold values from -0.109375 to 0.109375
- expert_up: bfloat16 [2, 16, 3072, 1024], P('pp', 'ep', None, 'tp'), may hold values from -0.109375 to 0.109375
- expert_down: bfloat16 [2, 16, 1024, 3072], P('pp', 'ep', 'tp'), may hold values from -0.1875 to 0.1875
Outputs:
- layer_out: bfloat16 [2, 2, 96, 3072], P('pp', None, 'ep')
The draws below stay inside these ranges and needn't reach their ends.
Inputs may be any that keep to these rules, and one draw needn't show every extreme that they name: `route_ids`: the 8 ids of a token differ. In each layer and microbatch, among the 6 tokens of one ep index no id is named by more than 2 tokens, a bound that some block reaches.
All inputs are finite; a program needn't handle non-finite values.
Results may differ from the reference program's by a relative error of at most 0.008.
Values may be sent and summed in bfloat16 or wider, within the bound.
No kernel may reach another device: no remote copies, remote signals or barrier semaphores. Data moves between devices by JAX's collectives and lax.ppermute only.
A program may use at most 128 MiB of HBM per device.

```python
import math
import jax
import jax.numpy as jnp
import numpy as np
from jax import lax

D = 3072
FFE = 1024
DFF = 6144
TOPK = 8
T_EP = 6
N_MB = 2
E = 16
E_ALL = 24
CAP = 2
MB = 96
N_EP = 16


def steps_of(own_key, extent, pieces, least, largest):
    def one(axis_at, parts):
        steps = jax.random.uniform(jax.random.fold_in(jax.random.fold_in(own_key, 6), axis_at), (parts,), jnp.float32, least / len(pieces), largest / len(pieces))
        return jnp.repeat(jnp.exp(steps), extent[axis_at] // parts).reshape((-1,) + (1,) * (len(extent) - axis_at - 1))

    factor_of = one(*pieces[0])
    for cut in pieces[1:]:
        factor_of = factor_of * one(*cut)
    return factor_of


def assign_block(rng, own, number, rows, amount, top, most, skew):
    order = jax.random.permutation(rng, amount)
    heavy_load, common = portions_of(amount, rows * top, most, skew, True), portions_of(amount, rows * top, most, skew, False)
    places = jnp.arange(amount)

    def named(sizes, rotation):
        used = int((sizes > 0).sum())
        fixed = max(1, used // 4)
        shifted = fixed + (places - fixed + rotation * (used - fixed)) % max(1, amount - fixed)
        return jnp.zeros((amount,), jnp.int32).at[order[jnp.where(places < fixed, places, shifted)]].set(jnp.asarray(sizes, jnp.int32))

    sizes = jnp.where(number % 4 == 0, named(heavy_load, number // 4), named(common, number - number // 4 - 1))
    mixed = jax.random.permutation(jax.random.fold_in(own, 3), amount)
    giver, sink = mixed[0:amount // 2 * 2:2], mixed[1:amount // 2 * 2:2]
    room = jnp.minimum(sizes[giver] - 1, most - sizes[sink]) // 2
    room = jnp.where((giver == order[0]) | (sink == order[0]) | (sizes[sink] == 0), 0, jnp.maximum(room, 0))
    shifted = jax.random.randint(jax.random.fold_in(own, 4), (amount // 2,), 0, 1 << 20) % (room + 1)
    sizes = sizes.at[giver].add(-shifted).at[sink].add(shifted)
    members = jnp.searchsorted(jnp.cumsum(sizes), jnp.arange(rows * top), side="right").astype(jnp.int32)
    table = members.reshape(top, rows).T
    table = table[jax.random.permutation(jax.random.fold_in(own, 1), rows)]
    rotation = jax.random.randint(jax.random.fold_in(own, 2), (rows, 1), 0, top)
    return jnp.take_along_axis(table, (jnp.arange(top)[None, :] + rotation) % top, axis=1)


def portions_of(amount, total, limit, lean, full):
    loads = [(1 << 20) // math.isqrt(grade ** lean) + 1 for grade in range(1, amount + 1)]
    largest = limit if full else min(limit, max(-(-total // amount), total * loads[0] // sum(loads)))
    least = 1 if total - largest >= amount - 1 else 0
    holding, rest = [largest] + [least] * (amount - 1), total - largest - least * (amount - 1)
    while rest > 0:
        candidates = [i for i in range(1, amount) if holding[i] < largest] or [i for i in range(1, amount) if holding[i] < limit]
        whole, remaining = sum([loads[i] for i in candidates]), rest
        for i in candidates:
            extra = min(limit - holding[i], max(1, remaining * loads[i] // whole), rest)
            holding[i] = holding[i] + extra
            rest = rest - extra
    return np.array(holding)


def bell_draw(key, shape, scale, limit, shards=(), kind=jnp.bfloat16):
    result = jax.random.normal(key, shape, jnp.float32) * scale
    if len(shards) > 0:
        result = steps_of(key, shape, shards, -0.22, 0.18) * result
    return jnp.clip(result, min=-limit, max=limit).astype(kind)


def setup_inputs(seed: int = 0) -> dict:
    keys = jax.random.split(jax.random.key(seed), 11)
    acts = bell_draw(keys[0], (N_MB, MB, D), 1.0, 6.0, ((1, 16),))
    route_ids_keys = jax.random.split(jax.random.fold_in(keys[1], 1), 2 * N_MB * MB // T_EP)
    route_ids_turns = jax.random.permutation(jax.random.fold_in(keys[1], 3), 2 * N_MB * MB // T_EP)
    route_ids = jax.vmap(lambda own, number: assign_block(jax.random.fold_in(keys[1], 2), own, number, T_EP, E_ALL, TOPK, CAP, 2))(route_ids_keys, route_ids_turns).reshape((2, N_MB, MB, TOPK))
    norm_gain = jnp.clip(1.0 + 0.1 * jax.random.normal(keys[2], (2, D), jnp.float32), 0.5, 1.5).astype(jnp.bfloat16)
    router = bell_draw(keys[3], (2, D, E_ALL), D ** -0.5, 0.109375, ((0, 2),))
    dense_gate = bell_draw(keys[4], (2, D, DFF), D ** -0.5, 0.109375, ((0, 2), (2, 16)))
    dense_up = bell_draw(keys[5], (2, D, DFF), D ** -0.5, 0.109375, ((0, 2), (2, 16)))
    dense_down = bell_draw(keys[6], (2, DFF, D), DFF ** -0.5, 0.078125, ((0, 2), (1, 16)))
    expert_gate = bell_draw(keys[7], (2, E, D, FFE), D ** -0.5, 0.109375, ((0, 2), (1, 16)))
    expert_up = bell_draw(keys[8], (2, E, D, FFE), D ** -0.5, 0.109375, ((0, 2), (1, 16)))
    expert_down = bell_draw(keys[9], (2, E, FFE, D), FFE ** -0.5, 0.1875, ((0, 2), (1, 16)))
    return {"acts": acts, "route_ids": route_ids, "norm_gain": norm_gain, "router": router, "dense_gate": dense_gate, "dense_up": dense_up, "dense_down": dense_down, "expert_gate": expert_gate, "expert_up": expert_up, "expert_down": expert_down}


def normalize(inputs, gain):
    widened = inputs.astype(jnp.float32)
    spread = lax.optimization_barrier(jnp.mean(widened * widened, axis=-1, keepdims=True))
    normed = (widened * lax.rsqrt(spread + 1e-06) * gain.astype(jnp.float32)).astype(jnp.bfloat16)
    return (widened, normed)

def gated_block(inputs, w_gate, w_up, w_down):
    gate_part = jnp.dot(inputs, w_gate, preferred_element_type=jnp.float32)
    up_part = jnp.dot(inputs, w_up, preferred_element_type=jnp.float32)
    hidden = (jax.nn.silu(gate_part) * up_part).astype(jnp.bfloat16)
    return jnp.dot(hidden, w_down, preferred_element_type=jnp.float32)

def choice_weights(normed, route_rows, router_w, n_real):
    n_total = router_w.shape[1]
    gates = jax.nn.sigmoid(jnp.dot(normed, router_w, preferred_element_type=jnp.float32))
    picked = (route_rows[:, :, None] == jnp.arange(n_total, dtype=jnp.int32)[None, None, :]).astype(jnp.float32)
    weights = lax.optimization_barrier(jnp.sum(picked * gates[:, None, :], axis=-1))
    zero_share = lax.optimization_barrier(jnp.sum(jnp.where(route_rows >= n_real, weights, jnp.float32(0.0)), axis=-1))
    return (weights, picked, zero_share)

def layer_ref(inputs, route_rows, gain, router_w, d_gate, d_up, d_down, e_gate, e_up, e_down):
    widened, normed = normalize(inputs, gain)
    n_real = e_gate.shape[0]
    weights, picked, zero_share = choice_weights(normed, route_rows, router_w, n_real)
    coef = jnp.einsum('tk,tke->te', weights, picked[:, :, :n_real], precision=lax.Precision.HIGHEST)
    dense = gated_block(normed, d_gate, d_up, d_down)
    token_count = inputs.shape[0]
    buffer_rows = min(token_count, N_EP * CAP)
    slot_range = jnp.arange(buffer_rows, dtype=jnp.float32)

    def one_expert(expert, total):
        hot = lax.optimization_barrier(jnp.sum((route_rows == expert).astype(jnp.float32), axis=-1))
        position = jnp.cumsum(hot) - hot
        select = hot[None, :] * (position[None, :] == slot_range[:, None]).astype(jnp.float32)
        chosen = jnp.dot(select.astype(jnp.bfloat16), normed, preferred_element_type=jnp.float32).astype(jnp.bfloat16)
        produced = gated_block(chosen, e_gate[expert], e_up[expert], e_down[expert])
        column = lax.dynamic_slice_in_dim(coef, expert, 1, 1)
        return total + jnp.dot(select.T, produced, precision=lax.Precision.HIGHEST) * column
    routed = lax.fori_loop(0, n_real, one_expert, jnp.zeros(widened.shape, jnp.float32))
    return (widened + dense + routed + zero_share[:, None] * normed.astype(jnp.float32)).astype(jnp.bfloat16)

def reference(acts, route_ids, norm_gain, router, dense_gate, dense_up, dense_down, expert_gate, expert_up, expert_down):
    first_section = []
    second_section = []
    for micro in range(N_MB):
        early = layer_ref(acts[micro], route_ids[0, micro], norm_gain[0], router[0], dense_gate[0], dense_up[0], dense_down[0], expert_gate[0], expert_up[0], expert_down[0])
        late = layer_ref(early, route_ids[1, micro], norm_gain[1], router[1], dense_gate[1], dense_up[1], dense_down[1], expert_gate[1], expert_up[1], expert_down[1])
        first_section.append(early)
        second_section.append(late)
    return jnp.stack([jnp.stack(first_section), jnp.stack(second_section)])
```

```python
import jax
import jax.numpy as jnp
from jax import lax
from jax.sharding import PartitionSpec as P


def exchange(blocks, axes):
    return lax.all_to_all(blocks, axes, split_axis=0, concat_axis=0, tiled=True)


def normalize(inputs, gain):
    widened = inputs.astype(jnp.float32)
    spread = jnp.mean(widened * widened, axis=-1, keepdims=True)
    normed = (widened * lax.rsqrt(spread + 1e-06) * gain.astype(jnp.float32)).astype(jnp.bfloat16)
    return (widened, normed)


def gated_block(inputs, w_gate, w_up, w_down):
    gate_part = jnp.dot(inputs, w_gate, preferred_element_type=jnp.float32)
    up_part = jnp.dot(inputs, w_up, preferred_element_type=jnp.float32)
    hidden = (jax.nn.silu(gate_part) * up_part).astype(jnp.bfloat16)
    return jnp.dot(hidden, w_down, preferred_element_type=jnp.float32)


def layer(inputs, ids, gain, router_w, dense, expert):
    rows, width = inputs.shape
    top_count = ids.shape[-1]
    n_groups = lax.axis_size("ep")
    n_pairs = lax.axis_size("tp")
    group_pos = lax.axis_index("ep")
    share = rows // n_pairs

    packed = jnp.concatenate([inputs, jnp.pad(ids, ((0, 0), (0, 128 - top_count))).astype(jnp.bfloat16)], axis=1)
    gathered = exchange(jnp.broadcast_to(packed[None], (n_groups, rows, width + 128)), "ep")
    gathered = gathered.reshape(n_groups * rows, width + 128)
    all_ids = gathered[:, width : width + top_count].astype(jnp.int32)
    _, all_normed = normalize(gathered[:, :width], gain)
    named = jnp.sum((all_ids == group_pos).astype(jnp.float32), axis=-1, keepdims=True)
    column = lax.dynamic_slice_in_dim(router_w, group_pos, 1, 1)
    gate = jax.nn.sigmoid(jnp.dot(all_normed, column, preferred_element_type=jnp.float32))
    partial = gated_block(all_normed, *dense) + (named * gate) * gated_block(all_normed, *expert)

    widened, normed = normalize(inputs, gain)
    gates = jax.nn.sigmoid(jnp.dot(normed, router_w, preferred_element_type=jnp.float32))
    id_range = jnp.arange(router_w.shape[1], dtype=jnp.int32)
    picked = jnp.sum((ids[:, :, None] == id_range[None, None, :]).astype(jnp.float32), axis=1)
    zero_share = jnp.sum(jnp.where(id_range[None, :] >= n_groups, picked * gates, 0.0), axis=-1, keepdims=True)
    base = widened + zero_share * normed.astype(jnp.float32)

    pieces = partial.astype(jnp.bfloat16).reshape(n_groups * n_pairs, share, width)
    received = exchange(pieces, ("ep", "tp"))
    own = lax.dynamic_slice_in_dim(base, lax.axis_index("tp") * share, share, 0)
    part = (own + jnp.sum(received.astype(jnp.float32), axis=0)).astype(jnp.bfloat16)
    return lax.all_gather(part, "tp", axis=0, tiled=True) if n_pairs > 1 else part


def on_device(
    acts,
    route_ids,
    norm_gain,
    router,
    dense_gate,
    dense_up,
    dense_down,
    expert_gate,
    expert_up,
    expert_down,
):
    n_micro, per_group, width = acts.shape
    n_sections = lax.axis_size("pp")
    section = lax.axis_index("pp")
    ids = route_ids[0].reshape(n_micro * per_group, -1)
    dense = (dense_gate[0], dense_up[0], dense_down[0])
    expert = (expert_gate[0, 0], expert_up[0, 0], expert_down[0, 0])

    current = acts.reshape(n_micro * per_group, width)
    result = current
    for phase in range(n_sections):
        result = lax.cond(
            section == phase,
            lambda held, fed: layer(fed, ids, norm_gain[0], router[0], dense, expert),
            lambda held, fed: held,
            result,
            current,
        )
        if phase + 1 < n_sections:
            current = lax.ppermute(result, "pp", [(phase, phase + 1)])
    return result.reshape(1, n_micro, per_group, width)


def solution(mesh):
    return jax.shard_map(
        on_device,
        mesh=mesh,
        in_specs=(
            P(None, "ep", None),
            P("pp", None, "ep", None),
            P("pp", None),
            P("pp", None, None),
            P("pp", None, ("ep", "tp")),
            P("pp", None, ("ep", "tp")),
            P("pp", ("ep", "tp"), None),
            P("pp", "ep", None, "tp"),
            P("pp", "ep", None, "tp"),
            P("pp", "ep", "tp", None),
        ),
        out_specs=P("pp", None, "ep", None),
        check_vma=False,
    )
```

```python
import math

import jax
import jax.numpy as jnp
from jax import lax
from jax.experimental import pallas as pl
from jax.experimental.pallas import tpu as pltpu
from jax.sharding import PartitionSpec as P

LANES = 128
SUBLANES = 8
MIB = 1 << 20
AHEAD = 8
WHOLE = pl.BlockSpec(memory_space=pltpu.VMEM)
SCALAR = pl.BlockSpec(memory_space=pltpu.SMEM)
OUTSIDE = pl.BlockSpec(memory_space=pl.ANY)


def exchange(blocks, axes):
    return lax.all_to_all(blocks, axes, split_axis=0, concat_axis=0, tiled=True)


def unfold(folded, parts):
    rows, width = folded.shape[0] // parts, folded.shape[1]
    return folded.reshape(parts, rows, width).swapaxes(0, 1).reshape(rows, parts * width)


def sigmoid(v):
    return 1.0 / (1.0 + jnp.exp(-v))


def across(a, b):
    return lax.dot_general(a, b, (((1,), (1,)), ((), ())), preferred_element_type=jnp.float32)


def column_cuts(total, size):
    return [(at, min(size, total - at)) for at in range(0, total, size)]


def pack_kernel(parts, x_ref, ids_ref, sent_ref, kept_ref, block_ref):
    n_micro, per_group, top_count = ids_ref.shape
    rows = n_micro * per_group
    span = block_ref.shape[1] - LANES
    block_ref[:, span:] = jnp.full((parts * rows, LANES), -1.0, jnp.float32)
    for m in range(n_micro):
        block_ref[m * per_group : (m + 1) * per_group, span : span + top_count] = ids_ref[m].astype(jnp.float32)
    if len(x_ref.shape) == 3:
        for m in range(n_micro):
            mine = x_ref[m].astype(jnp.float32)
            for p in range(parts):
                at = p * rows + m * per_group
                block_ref[at : at + per_group, :span] = mine[:, p * span : (p + 1) * span]
    else:
        block_ref[:, :span] = x_ref[...].astype(jnp.float32)
    block = block_ref[...].astype(jnp.bfloat16)
    kept_ref[...] = block
    for g in range(sent_ref.shape[0]):
        sent_ref[g] = block


def base_kernel(n_real, top_count, parts, kept_ref, gain_ref, router_ref, base_ref):
    rows, span = base_ref.shape[0] // parts, base_ref.shape[1]
    block = kept_ref[...].astype(jnp.float32)
    pieces = [block[p * rows : (p + 1) * rows, :span] for p in range(parts)]
    ids = block[:rows, span:]
    spread = sum(jnp.sum(v * v, axis=-1, keepdims=True) for v in pieces) / (parts * span)
    scale = lax.rsqrt(spread + 1e-06)
    gains = [gain_ref[:, p * span : (p + 1) * span].astype(jnp.float32) for p in range(parts)]
    normed = [(v * scale * gain).astype(jnp.bfloat16) for v, gain in zip(pieces, gains)]
    logits = sum(across(v, router_ref[:, p * span : (p + 1) * span]) for p, v in enumerate(normed))
    gates = sigmoid(logits)
    id_range = lax.broadcasted_iota(jnp.int32, gates.shape, 1)
    named = id_range.astype(jnp.float32)
    picked = sum((ids[:, k : k + 1] == named).astype(jnp.float32) for k in range(top_count))
    share = jnp.sum(jnp.where(id_range >= n_real, picked * gates, 0.0), axis=-1, keepdims=True)
    for p in range(parts):
        base_ref[p * rows : (p + 1) * rows, :] = pieces[p] + share * normed[p].astype(jnp.float32)


def layer_kernel(rows, parts, place_ref, all_ref, gain_ref, router_ref, *refs):
    sources, out_ref = refs[:6], refs[6]
    d_gate, d_up, d_down, e_gate, e_up, e_down = refs[7:13]
    normed_ref, coef_ref, d_hidden, e_hidden, value_ref, sems = refs[13:]
    n_groups, _, padded = all_ref.shape
    span = out_ref.shape[2]
    width = parts * span
    place = place_ref[0]
    unit = 16 // math.gcd(rows, 16)
    unit = unit if n_groups % unit == 0 else n_groups

    plan = []
    for at, size in column_cuts(d_gate.shape[1], 512):
        plan += [(0, d_gate, at, size), (1, d_up, at, size)]
    for at, size in column_cuts(e_gate.shape[1], 256):
        plan += [(3, e_gate, at, size), (4, e_up, at, size)]
    for at, size in column_cuts(width, 768):
        plan += [(2, d_down, at, size), (5, e_down, at, size)]
    copies = {}
    for i, (which, held, at, size) in enumerate(plan):
        source = sources[which].at[:, pl.ds(at, size)]
        copies[which, at] = (i, pltpu.make_async_copy(source, held.at[:, pl.ds(at, size)], sems.at[i]))
    order = list(copies.values())
    for i, copy in order[:AHEAD]:
        copy.start()

    def arrive(which, at):
        i, copy = copies[which, at]
        copy.wait()
        if i + AHEAD < len(order):
            order[i + AHEAD][1].start()

    def load(step, carry):
        start = pl.multiple_of(step * unit * rows, 16)
        blocks = [all_ref[step * unit + u].astype(jnp.float32) for u in range(unit)]
        pieces = [
            jnp.concatenate([b[p * rows : (p + 1) * rows, :span] for b in blocks], axis=0) for p in range(parts)
        ]
        ids = jnp.concatenate([b[:rows, span:] for b in blocks], axis=0)
        named = jnp.sum((ids == place.astype(jnp.float32)).astype(jnp.float32), axis=-1, keepdims=True)
        spread = sum(jnp.sum(v * v, axis=-1, keepdims=True) for v in pieces) / width
        scale = lax.rsqrt(spread + 1e-06)
        for p, v in enumerate(pieces):
            gain = gain_ref[:, p * span : (p + 1) * span].astype(jnp.float32)
            normed_ref[pl.ds(start, unit * rows), p * span : (p + 1) * span] = (v * scale * gain).astype(jnp.bfloat16)
        coef_ref[pl.ds(start, unit * rows), :] = jnp.broadcast_to(named, (unit * rows, LANES))
        return carry

    lax.fori_loop(0, n_groups // unit, load, 0)

    logits = across(normed_ref[...], router_ref[...])
    mine = lax.broadcasted_iota(jnp.int32, logits.shape, 1) == place
    gate = jnp.sum(jnp.where(mine, sigmoid(logits), 0.0), axis=-1, keepdims=True)
    coef_ref[...] = coef_ref[...] * gate

    def hidden(first, w_gate, w_up, target, size):
        for at, size in column_cuts(target.shape[1], size):
            cols = slice(at, at + size)
            arrive(first, at)
            gate_part = jnp.dot(normed_ref[...], w_gate[:, cols], preferred_element_type=jnp.float32)
            arrive(first + 1, at)
            up_part = jnp.dot(normed_ref[...], w_up[:, cols], preferred_element_type=jnp.float32)
            target[:, cols] = (gate_part * sigmoid(gate_part) * up_part).astype(jnp.bfloat16)

    hidden(0, d_gate, d_up, d_hidden, 512)
    hidden(3, e_gate, e_up, e_hidden, 256)
    for at, size in column_cuts(width, 768):
        arrive(2, at)
        arrive(5, at)
        for sub, step in column_cuts(size, 256):
            cols = slice(at + sub, at + sub + step)
            dense = jnp.dot(d_hidden[...], d_down[:, cols], preferred_element_type=jnp.float32)
            routed = jnp.dot(e_hidden[...], e_down[:, cols], preferred_element_type=jnp.float32)
            value_ref[:, cols] = dense + coef_ref[:, :1] * routed

    def pack(step, carry):
        start = pl.multiple_of(step * unit * rows, 16)
        tall = value_ref[pl.ds(start, unit * rows), :]
        for u in range(unit):
            mine = tall[u * rows : (u + 1) * rows]
            block = jnp.concatenate([mine[:, p * span : (p + 1) * span] for p in range(parts)], axis=0)
            out_ref[step * unit + u] = block.astype(out_ref.dtype)
        return carry

    lax.fori_loop(0, n_groups // unit, pack, 0)


def combine_kernel(parts, got_ref, base_ref, folded_ref, flat_ref, total_ref):
    n_micro, per_group, width = flat_ref.shape
    rows, span = n_micro * per_group, base_ref.shape[1]
    total = base_ref[...]
    for g in range(got_ref.shape[0]):
        total = total + got_ref[g].astype(jnp.float32)
    folded_ref[...] = total.astype(jnp.bfloat16)
    total_ref[...] = total
    for m in range(n_micro):
        for p in range(parts):
            at = p * rows + m * per_group
            flat_ref[m, :, p * span : (p + 1) * span] = total_ref[at : at + per_group, :].astype(jnp.bfloat16)


def layer(fed, ids, gain, router_t, weights, parts):
    n_micro, per_group, top_count = ids.shape
    n_groups = lax.axis_size("ep")
    n_pairs = lax.axis_size("tp")
    place = lax.axis_index("ep")
    width = gain.shape[1]
    rows, span = n_micro * per_group, width // parts
    tall, wide = parts * rows, span + LANES
    count = n_groups * rows

    sent, kept = pl.pallas_call(
        lambda *refs: pack_kernel(parts, *refs),
        out_shape=[
            jax.ShapeDtypeStruct((n_groups, tall, wide), jnp.bfloat16),
            jax.ShapeDtypeStruct((tall, wide), jnp.bfloat16),
        ],
        in_specs=[WHOLE, WHOLE],
        out_specs=[WHOLE, WHOLE],
        scratch_shapes=[pltpu.VMEM((tall, wide), jnp.float32)],
        compiler_params=pltpu.CompilerParams(vmem_limit_bytes=16 * MIB),
        name="pack",
    )(fed, ids)
    gathered = exchange(sent, "ep")

    base = pl.pallas_call(
        lambda *refs: base_kernel(n_groups, top_count, parts, *refs),
        out_shape=jax.ShapeDtypeStruct((tall, span), jnp.float32),
        in_specs=[WHOLE] * 3,
        out_specs=WHOLE,
        compiler_params=pltpu.CompilerParams(vmem_limit_bytes=8 * MIB),
        cost_estimate=pl.CostEstimate(flops=int(1e8), bytes_accessed=int(1e6), transcendentals=0),
        name="base",
    )(kept, gain, router_t)

    n_dense, n_expert = weights[0].shape[1], weights[3].shape[1]
    partial = pl.pallas_call(
        lambda *refs: layer_kernel(rows, parts, *refs),
        out_shape=jax.ShapeDtypeStruct((n_groups, tall, span), jnp.bfloat16),
        in_specs=[SCALAR] + [WHOLE] * 3 + [OUTSIDE] * 6,
        out_specs=WHOLE,
        scratch_shapes=[pltpu.VMEM(w.shape, w.dtype) for w in weights]
        + [
            pltpu.VMEM((count, width), jnp.bfloat16),
            pltpu.VMEM((count, LANES), jnp.float32),
            pltpu.VMEM((count, n_dense), jnp.bfloat16),
            pltpu.VMEM((count, n_expert), jnp.bfloat16),
            pltpu.VMEM((count, width), jnp.float32),
            pltpu.SemaphoreType.DMA((64,)),
        ],
        compiler_params=pltpu.CompilerParams(vmem_limit_bytes=54 * MIB),
        cost_estimate=pl.CostEstimate(
            flops=6 * count * width * (n_dense + n_expert),
            bytes_accessed=6 * width * (n_dense + n_expert),
            transcendentals=0,
        ),
        name="layer",
    )(place.reshape(1).astype(jnp.int32), gathered, gain, router_t, *weights)

    share = tall // n_pairs
    received = exchange(partial.reshape(n_groups * n_pairs, share, span), ("ep", "tp"))
    if n_pairs > 1:
        kept_base = lax.dynamic_slice_in_dim(base, lax.axis_index("tp") * share, share, 0)
        part = (kept_base + jnp.sum(received.astype(jnp.float32), axis=0)).astype(jnp.bfloat16)
        folded = lax.all_gather(part, "tp", axis=0, tiled=True)
        return folded, unfold(folded, parts).reshape(n_micro, per_group, width)
    return pl.pallas_call(
        lambda *refs: combine_kernel(parts, *refs),
        out_shape=[
            jax.ShapeDtypeStruct((tall, span), jnp.bfloat16),
            jax.ShapeDtypeStruct((n_micro, per_group, width), jnp.bfloat16),
        ],
        in_specs=[WHOLE, WHOLE],
        out_specs=[WHOLE, WHOLE],
        scratch_shapes=[pltpu.VMEM((tall, span), jnp.float32)],
        compiler_params=pltpu.CompilerParams(vmem_limit_bytes=8 * MIB),
        name="combine",
    )(received, base)


def on_device(
    acts,
    route_ids,
    norm_gain,
    router,
    dense_gate,
    dense_up,
    dense_down,
    expert_gate,
    expert_up,
    expert_down,
):
    n_micro, per_group, width = acts.shape
    n_sections = lax.axis_size("pp")
    section = lax.axis_index("pp")
    rows = n_micro * per_group
    parts = SUBLANES // math.gcd(rows, SUBLANES)
    weights = (
        dense_gate[0],
        dense_up[0],
        dense_down[0],
        expert_gate[0, 0],
        expert_up[0, 0],
        expert_down[0, 0],
    )
    router_t = router[0].T

    fed = acts
    folded, flat = jnp.zeros((parts * rows, width // parts), jnp.bfloat16), acts
    for phase in range(n_sections):
        folded, flat = lax.cond(
            section == phase,
            lambda held, given: layer(given, route_ids[0], norm_gain, router_t, weights, parts),
            lambda held, given: held,
            (folded, flat),
            fed,
        )
        if phase + 1 < n_sections:
            fed = lax.ppermute(folded, "pp", [(phase, phase + 1)])
    return flat[None]


def solution(mesh):
    return jax.shard_map(
        on_device,
        mesh=mesh,
        in_specs=(
            P(None, "ep", None),
            P("pp", None, "ep", None),
            P("pp", None),
            P("pp", None, None),
            P("pp", None, ("ep", "tp")),
            P("pp", None, ("ep", "tp")),
            P("pp", ("ep", "tp"), None),
            P("pp", "ep", None, "tp"),
            P("pp", "ep", None, "tp"),
            P("pp", "ep", "tp", None),
        ),
        out_specs=P("pp", None, "ep", None),
        check_vma=False,
    )
```

```python
import math

import jax
import jax.numpy as jnp
from jax import lax
from jax.experimental import pallas as pl
from jax.experimental.pallas import tpu as pltpu
from jax.sharding import PartitionSpec as P

LANES = 128
SUBLANES = 8
MIB = 1 << 20
FLIGHT = 12 * MIB
PIECE = 3 * MIB // 4
HIDDEN = 256
OUT = 512
WHOLE = pl.BlockSpec(memory_space=pltpu.VMEM)
SCALAR = pl.BlockSpec(memory_space=pltpu.SMEM)
OUTSIDE = pl.BlockSpec(memory_space=pl.ANY)


def exchange(blocks, axes):
    return lax.all_to_all(blocks, axes, split_axis=0, concat_axis=0, tiled=True)


def unfold(folded, parts):
    tall = folded.shape[0]
    lines = []
    for at, _, height in regions(tall // parts, parts):
        pieces = [folded[at + p * height : at + (p + 1) * height] for p in range(parts)]
        lines.append(jnp.concatenate(pieces, axis=1))
    return jnp.concatenate(lines, axis=0)


def sigmoid(v):
    return 1.0 / (1.0 + jnp.exp(-v))


def across(a, b):
    return lax.dot_general(a, b, (((1,), (1,)), ((), ())), preferred_element_type=jnp.float32)


def spread_of(pieces):
    count = sum(v.shape[1] for v in pieces)
    return sum(jnp.sum(v * v, axis=-1, keepdims=True) for v in pieces) / count


def regions(rows, parts):
    even = rows // SUBLANES * SUBLANES
    found = [(0, 0, even), (parts * even, even, rows - even)]
    return [region for region in found if region[2] > 0]


def place_in_block(rows, parts, part, row):
    for at, first, height in regions(rows, parts):
        if first <= row < first + height:
            return at + part * height + row - first


def pair_shapes(width, count):
    if count % LANES == 0:
        return [(width, 2 * count), (SUBLANES, LANES)]
    return [(width, count)] * 2


def refs_joined(held, source):
    return held.shape[1] == 2 * source.shape[1]


def column_cuts(total, size):
    return [(at, min(size, total - at)) for at in range(0, total, size)]


def pack_kernel(parts, x_ref, ids_ref, sent_ref, kept_ref, block_ref):
    per_group, n_micro, top_count = ids_ref.shape
    rows = n_micro * per_group
    span = block_ref.shape[1] - LANES
    step = math.gcd(n_micro, SUBLANES)
    block_ref[:, span:] = jnp.full((parts * rows, LANES), -1.0, jnp.float32)
    for i in range(per_group):
        ids = ids_ref[i].astype(jnp.float32)
        for m in range(0, n_micro, step):
            at = place_in_block(rows, parts, 0, i * n_micro + m)
            block_ref[at : at + step, span : span + top_count] = ids[m : m + step]
    if len(x_ref.shape) == 3:
        for i in range(per_group):
            mine = x_ref[i].astype(jnp.float32)
            for m in range(0, n_micro, step):
                for p in range(parts):
                    at = place_in_block(rows, parts, p, i * n_micro + m)
                    block_ref[at : at + step, :span] = mine[m : m + step, p * span : (p + 1) * span]
    else:
        block_ref[:, :span] = x_ref[...].astype(jnp.float32)
    block = block_ref[...].astype(jnp.bfloat16)
    kept_ref[...] = block
    for g in range(sent_ref.shape[0]):
        sent_ref[g] = block


def base_kernel(n_real, top_count, parts, kept_ref, gain_ref, router_ref, base_ref):
    span = base_ref.shape[1]
    gains = [gain_ref[:, p * span : (p + 1) * span].astype(jnp.float32) for p in range(parts)]
    block = kept_ref[...].astype(jnp.float32)
    for at, _, height in regions(base_ref.shape[0] // parts, parts):
        pieces = [block[at + p * height : at + (p + 1) * height, :span] for p in range(parts)]
        ids = block[at : at + height, span:]
        scale = lax.rsqrt(spread_of(pieces) + 1e-06)
        normed = [(v * scale * gain).astype(jnp.bfloat16) for v, gain in zip(pieces, gains)]
        logits = sum(across(v, router_ref[:, p * span : (p + 1) * span]) for p, v in enumerate(normed))
        gates = sigmoid(logits)
        id_range = lax.broadcasted_iota(jnp.int32, gates.shape, 1)
        named = id_range.astype(jnp.float32)
        picked = sum((ids[:, k : k + 1] == named).astype(jnp.float32) for k in range(top_count))
        share = jnp.sum(jnp.where(id_range >= n_real, picked * gates, 0.0), axis=-1, keepdims=True)
        for p in range(parts):
            rows = slice(at + p * height, at + (p + 1) * height)
            base_ref[rows, :] = pieces[p] + share * normed[p].astype(jnp.float32)


def layer_kernel(rows, parts, place_ref, all_ref, gain_ref, router_ref, *refs):
    sources, out_ref = refs[:6], refs[6]
    held = refs[7:13]
    d_down, e_down = held[2], held[5]
    normed_ref, coef_ref, d_hidden, e_hidden, value_ref, stage_ref, sems, out_sems = refs[13:]
    n_groups = all_ref.shape[0]
    span = out_ref.shape[2]
    width = parts * span
    place = place_ref[0]
    unit = 16 // math.gcd(rows, 16)
    unit = unit if n_groups % unit == 0 else n_groups

    out_cuts = column_cuts(span, OUT)
    if span % OUT == 0 and OUT % (2 * LANES) == 0:
        out_cuts = out_cuts[:-1] + [(span - OUT, OUT // 2), (span - OUT // 2, OUT // 2)]
    plan = []
    for which, hidden_ref in ((0, d_hidden), (3, e_hidden)):
        joined = hidden_ref.shape[1] % LANES == 0
        for at, size in column_cuts(hidden_ref.shape[1], HIDDEN):
            spots = (2 * at, 2 * at + size) if joined else (at, at)
            plan += [(which, at, spots[0], size), (which + 1, at, spots[1], size)]
    for at, size in out_cuts:
        plan += [(which, p * span + at, p * span + at, size) for which in (2, 5) for p in range(parts)]
    held = tuple(
        held[i - 1] if i in (1, 4) and refs_joined(held[i - 1], sources[i]) else h for i, h in enumerate(held)
    )
    order, owned, volume, total = [], {}, [], 0
    for which, at, put, size in plan:
        height = held[which].shape[0]
        pieces = max(1, height * size * 2 // PIECE)
        pieces = pieces if height % pieces == 0 and height // pieces % 16 == 0 else 1
        owned[which, at] = range(len(order), len(order) + pieces)
        for k in range(pieces):
            lines = pl.ds(k * (height // pieces), height // pieces)
            source, target = sources[which].at[lines, pl.ds(at, size)], held[which].at[lines, pl.ds(put, size)]
            order.append(pltpu.make_async_copy(source, target, sems.at[len(order)]))
            total += height // pieces * size * 2
            volume.append(total)
    begun = [0]

    def start_until(limit):
        while begun[0] < len(order) and volume[begun[0]] <= limit:
            order[begun[0]].start()
            begun[0] += 1

    start_until(max(FLIGHT, volume[0]))

    def arrive(which, at):
        for i in owned[which, at]:
            order[i].wait()
            start_until(volume[i] + FLIGHT)

    def load(step, carry):
        blocks = [all_ref[step * unit + u].astype(jnp.float32) for u in range(unit)]
        for at, first, height in regions(rows, parts):
            start = pl.multiple_of(n_groups * first + step * unit * height, 16)
            here = pl.ds(start, unit * height)
            pieces = [
                jnp.concatenate([b[at + p * height : at + (p + 1) * height, :span] for b in blocks], axis=0)
                for p in range(parts)
            ]
            ids = jnp.concatenate([b[at : at + height, span:] for b in blocks], axis=0)
            named = jnp.sum((ids == place.astype(jnp.float32)).astype(jnp.float32), axis=-1, keepdims=True)
            scale = lax.rsqrt(spread_of(pieces) + 1e-06)
            for p, v in enumerate(pieces):
                gain = gain_ref[:, p * span : (p + 1) * span].astype(jnp.float32)
                normed_ref[here, p * span : (p + 1) * span] = (v * scale * gain).astype(jnp.bfloat16)
            coef_ref[here, :] = jnp.broadcast_to(named, (unit * height, LANES))
        return carry

    lax.fori_loop(0, n_groups // unit, load, 0)

    logits = across(normed_ref[...], router_ref[...])
    mine = lax.broadcasted_iota(jnp.int32, logits.shape, 1) == place
    gate = jnp.sum(jnp.where(mine, sigmoid(logits), 0.0), axis=-1, keepdims=True)
    coef_ref[...] = coef_ref[...] * gate

    def hidden(which, target):
        joined = target.shape[1] % LANES == 0
        for at, size in column_cuts(target.shape[1], HIDDEN):
            arrive(which, at)
            arrive(which + 1, at)
            if joined:
                pair = jnp.dot(
                    normed_ref[...], held[which][:, 2 * at : 2 * (at + size)], preferred_element_type=jnp.float32
                )
                gate_part, up_part = pair[:, :size], pair[:, size:]
            else:
                gate_part, up_part = (
                    jnp.dot(normed_ref[...], held[w][:, at : at + size], preferred_element_type=jnp.float32)
                    for w in (which, which + 1)
                )
            target[:, at : at + size] = (gate_part * sigmoid(gate_part) * up_part).astype(jnp.bfloat16)

    hidden(0, d_hidden)
    hidden(3, e_hidden)

    leaving = []
    for at, size in out_cuts:
        for which in (2, 5):
            for p in range(parts):
                arrive(which, p * span + at)
        for p in range(parts):
            cols = slice(p * span + at, p * span + at + size)
            dense = jnp.dot(d_hidden[...], d_down[:, cols], preferred_element_type=jnp.float32)
            routed = jnp.dot(e_hidden[...], e_down[:, cols], preferred_element_type=jnp.float32)
            value_ref[:, p * OUT : p * OUT + size] = dense + coef_ref[:, :1] * routed

        def pack(step, carry):
            rows_of = []
            for _, first, height in regions(rows, parts):
                start = pl.multiple_of(n_groups * first + step * unit * height, SUBLANES)
                rows_of.append((height, value_ref[pl.ds(start, unit * height), :]))
            for u in range(unit):
                pieces = [
                    tall[u * height : (u + 1) * height, p * OUT : p * OUT + size]
                    for height, tall in rows_of
                    for p in range(parts)
                ]
                block = jnp.concatenate(pieces, axis=0).astype(out_ref.dtype)
                stage_ref[step * unit + u, :, at : at + size] = block
            return carry

        lax.fori_loop(0, n_groups // unit, pack, 0)
        cols = pl.ds(at, size)
        leaving.append(pltpu.make_async_copy(stage_ref.at[:, :, cols], out_ref.at[:, :, cols], out_sems.at[len(leaving)]))
        leaving[-1].start()
    for copy in leaving:
        copy.wait()


def combine_kernel(parts, got_ref, base_ref, folded_ref, flat_ref, total_ref):
    per_group, n_micro, width = flat_ref.shape
    rows, span = n_micro * per_group, base_ref.shape[1]
    total = base_ref[...]
    for g in range(got_ref.shape[0]):
        total = total + got_ref[g].astype(jnp.float32)
    folded_ref[...] = total.astype(jnp.bfloat16)
    total_ref[...] = total
    step = math.gcd(n_micro, SUBLANES)
    for i in range(per_group):
        for m in range(0, n_micro, step):
            for p in range(parts):
                at = place_in_block(rows, parts, p, i * n_micro + m)
                cols = slice(p * span, (p + 1) * span)
                flat_ref[i, m : m + step, cols] = total_ref[at : at + step, :].astype(jnp.bfloat16)


def layer(fed, ids, gain, router_t, weights, parts):
    per_group, n_micro, top_count = ids.shape
    n_groups = lax.axis_size("ep")
    n_pairs = lax.axis_size("tp")
    place = lax.axis_index("ep")
    width = gain.shape[1]
    rows, span = n_micro * per_group, width // parts
    tall, wide = parts * rows, span + LANES
    count = n_groups * rows

    sent, kept = pl.pallas_call(
        lambda *refs: pack_kernel(parts, *refs),
        out_shape=[
            jax.ShapeDtypeStruct((n_groups, tall, wide), jnp.bfloat16),
            jax.ShapeDtypeStruct((tall, wide), jnp.bfloat16),
        ],
        in_specs=[WHOLE, WHOLE],
        out_specs=[WHOLE, WHOLE],
        scratch_shapes=[pltpu.VMEM((tall, wide), jnp.float32)],
        compiler_params=pltpu.CompilerParams(vmem_limit_bytes=16 * MIB),
        name="pack",
    )(fed, ids)
    gathered = exchange(sent, "ep")

    base = pl.pallas_call(
        lambda *refs: base_kernel(n_groups, top_count, parts, *refs),
        out_shape=jax.ShapeDtypeStruct((tall, span), jnp.float32),
        in_specs=[WHOLE] * 3,
        out_specs=WHOLE,
        compiler_params=pltpu.CompilerParams(vmem_limit_bytes=8 * MIB),
        cost_estimate=pl.CostEstimate(flops=int(1e8), bytes_accessed=int(1e6), transcendentals=0),
        name="base",
    )(kept, gain, router_t)

    n_dense, n_expert = weights[0].shape[1], weights[3].shape[1]
    partial = pl.pallas_call(
        lambda *refs: layer_kernel(rows, parts, *refs),
        out_shape=jax.ShapeDtypeStruct((n_groups, tall, span), jnp.bfloat16),
        in_specs=[SCALAR] + [WHOLE] * 3 + [OUTSIDE] * 6,
        out_specs=OUTSIDE,
        scratch_shapes=[
            *(pltpu.VMEM(shape, jnp.bfloat16) for shape in pair_shapes(width, n_dense)),
            pltpu.VMEM((n_dense, width), jnp.bfloat16),
            *(pltpu.VMEM(shape, jnp.bfloat16) for shape in pair_shapes(width, n_expert)),
            pltpu.VMEM((n_expert, width), jnp.bfloat16),
            pltpu.VMEM((count, width), jnp.bfloat16),
            pltpu.VMEM((count, LANES), jnp.float32),
            pltpu.VMEM((count, n_dense), jnp.bfloat16),
            pltpu.VMEM((count, n_expert), jnp.bfloat16),
            pltpu.VMEM((count, parts * OUT), jnp.float32),
            pltpu.VMEM((n_groups, tall, span), jnp.bfloat16),
            pltpu.SemaphoreType.DMA((128,)),
            pltpu.SemaphoreType.DMA((16,)),
        ],
        compiler_params=pltpu.CompilerParams(vmem_limit_bytes=50 * MIB),
        cost_estimate=pl.CostEstimate(
            flops=6 * count * width * (n_dense + n_expert),
            bytes_accessed=6 * width * (n_dense + n_expert),
            transcendentals=0,
        ),
        name="layer",
    )(place.reshape(1).astype(jnp.int32), gathered, gain, router_t, *weights)

    share = tall // n_pairs
    received = exchange(partial.reshape(n_groups * n_pairs, share, span), ("ep", "tp"))
    if n_pairs > 1:
        kept_base = lax.dynamic_slice_in_dim(base, lax.axis_index("tp") * share, share, 0)
        part = (kept_base + jnp.sum(received.astype(jnp.float32), axis=0)).astype(jnp.bfloat16)
        folded = lax.all_gather(part, "tp", axis=0, tiled=True)
        return folded, unfold(folded, parts).reshape(per_group, n_micro, width)
    return pl.pallas_call(
        lambda *refs: combine_kernel(parts, *refs),
        out_shape=[
            jax.ShapeDtypeStruct((tall, span), jnp.bfloat16),
            jax.ShapeDtypeStruct((per_group, n_micro, width), jnp.bfloat16),
        ],
        in_specs=[WHOLE, WHOLE],
        out_specs=[WHOLE, WHOLE],
        scratch_shapes=[pltpu.VMEM((tall, span), jnp.float32)],
        compiler_params=pltpu.CompilerParams(vmem_limit_bytes=8 * MIB),
        name="combine",
    )(received, base)


def on_device(
    acts,
    route_ids,
    norm_gain,
    router,
    dense_gate,
    dense_up,
    dense_down,
    expert_gate,
    expert_up,
    expert_down,
):
    n_micro, per_group, width = acts.shape
    n_sections = lax.axis_size("pp")
    section = lax.axis_index("pp")
    rows = n_micro * per_group
    parts = SUBLANES // math.gcd(rows, SUBLANES)
    weights = (
        dense_gate[0],
        dense_up[0],
        dense_down[0],
        expert_gate[0, 0],
        expert_up[0, 0],
        expert_down[0, 0],
    )
    router_t = router[0].T

    fed = acts.swapaxes(0, 1)
    ids = route_ids[0].swapaxes(0, 1)
    kept = None
    for phase in range(n_sections):
        folded, flat = lax.cond(
            section == phase,
            lambda held, given: layer(given, ids, norm_gain, router_t, weights, parts),
            lambda held, given: held or (
                jnp.zeros((parts * rows, width // parts), jnp.bfloat16),
                jnp.zeros((per_group, n_micro, width), jnp.bfloat16),
            ),
            kept,
            fed,
        )
        kept = (folded, flat)
        if phase + 1 < n_sections:
            fed = lax.ppermute(folded, "pp", [(phase, phase + 1)])
    return flat.swapaxes(0, 1)[None]


def solution(mesh):
    return jax.shard_map(
        on_device,
        mesh=mesh,
        in_specs=(
            P(None, "ep", None),
            P("pp", None, "ep", None),
            P("pp", None),
            P("pp", None, None),
            P("pp", None, ("ep", "tp")),
            P("pp", None, ("ep", "tp")),
            P("pp", ("ep", "tp"), None),
            P("pp", "ep", None, "tp"),
            P("pp", "ep", None, "tp"),
            P("pp", "ep", "tp", None),
        ),
        out_specs=P("pp", None, "ep", None),
        check_vma=False,
    )
```

```python
import math

import jax
import jax.numpy as jnp
from jax import lax
from jax.experimental import pallas as pl
from jax.experimental.pallas import tpu as pltpu
from jax.sharding import PartitionSpec as P

LANES = 128
SUBLANES = 8
MIB = 1 << 20
FLIGHT = 12 * MIB
PIECE = 3 * MIB // 4
HIDDEN = 256
OUT = 512
REFS = 21
WHOLE = pl.BlockSpec(memory_space=pltpu.VMEM)
SCALAR = pl.BlockSpec(memory_space=pltpu.SMEM)
OUTSIDE = pl.BlockSpec(memory_space=pl.ANY)


def exchange(blocks, axes):
    return lax.all_to_all(blocks, axes, split_axis=0, concat_axis=0, tiled=True)


def unfold(folded, parts):
    tall = folded.shape[0]
    lines = []
    for at, _, height in regions(tall // parts, parts):
        pieces = [folded[at + p * height : at + (p + 1) * height] for p in range(parts)]
        lines.append(jnp.concatenate(pieces, axis=1))
    return jnp.concatenate(lines, axis=0)


def sigmoid(v):
    return 1.0 / (1.0 + jnp.exp(-v))


def across(a, b):
    return lax.dot_general(a, b, (((1,), (1,)), ((), ())), preferred_element_type=jnp.float32)


def spread_of(pieces):
    count = sum(v.shape[1] for v in pieces)
    return sum(jnp.sum(v * v, axis=-1, keepdims=True) for v in pieces) / count


def regions(rows, parts):
    even = rows // SUBLANES * SUBLANES
    found = [(0, 0, even), (parts * even, even, rows - even)]
    return [region for region in found if region[2] > 0]


def place_in_block(rows, parts, part, row):
    for at, first, height in regions(rows, parts):
        if first <= row < first + height:
            return at + part * height + row - first


def pair_shapes(width, count):
    if count % LANES == 0:
        return [(width, 2 * count), (SUBLANES, LANES)]
    return [(width, count)] * 2


def refs_joined(held, source):
    return held.shape[1] == 2 * source.shape[1]


def column_cuts(total, size):
    return [(at, min(size, total - at)) for at in range(0, total, size)]


def write_tags(ids_ref, rows, parts, tags_ref):
    per_group, n_micro, top_count = ids_ref.shape
    step = math.gcd(n_micro, SUBLANES)
    tags_ref[...] = jnp.full(tags_ref.shape, -1.0, jnp.float32)
    for i in range(per_group):
        ids = ids_ref[i].astype(jnp.float32)
        for m in range(0, n_micro, step):
            at = place_in_block(rows, parts, 0, i * n_micro + m)
            tags_ref[at : at + step, :top_count] = ids[m : m + step]


def tags_kernel(parts, ids_ref, sent_ref, kept_ref, tags_ref):
    write_tags(ids_ref, tags_ref.shape[0] // parts, parts, tags_ref)
    block = tags_ref[...].astype(jnp.bfloat16)
    kept_ref[...] = block
    for g in range(sent_ref.shape[0]):
        sent_ref[g] = block


def settle_kernel(tags_ref, out_ref, sem):
    copy = pltpu.make_async_copy(tags_ref, out_ref, sem)
    copy.start()
    copy.wait()


def first_pack_kernel(parts, x_hbm, ids_hbm, sent_ref, kept_ref, kept_tags_ref, x_ref, ids_ref, tags_ref, block_ref, sems):
    copies = [
        pltpu.make_async_copy(x_hbm, x_ref, sems.at[0]),
        pltpu.make_async_copy(ids_hbm, ids_ref, sems.at[1]),
    ]
    for copy in copies:
        copy.start()
    for copy in copies:
        copy.wait()
    per_group, n_micro, _ = x_ref.shape
    rows, span = per_group * n_micro, block_ref.shape[1]
    step = math.gcd(n_micro, SUBLANES)
    write_tags(ids_ref, rows, parts, tags_ref)
    for i in range(per_group):
        mine = x_ref[i].astype(jnp.float32)
        for m in range(0, n_micro, step):
            for p in range(parts):
                at = place_in_block(rows, parts, p, i * n_micro + m)
                block_ref[at : at + step, :] = mine[m : m + step, p * span : (p + 1) * span]
    block, tags = block_ref[...].astype(jnp.bfloat16), tags_ref[...].astype(jnp.bfloat16)
    kept_ref[...] = block
    kept_tags_ref[...] = tags
    for g in range(sent_ref.shape[0]):
        sent_ref[g, :, :span] = block
        sent_ref[g, :, span:] = tags


def later_pack_kernel(x_ref, sent_ref):
    for g in range(sent_ref.shape[0]):
        sent_ref[g] = x_ref[...]


def base_kernel(n_real, top_count, parts, kept_ref, tags_ref, gain_ref, router_ref, base_ref, blank_ref):
    blank_ref[...] = jnp.zeros(blank_ref.shape, blank_ref.dtype)
    span = base_ref.shape[1]
    gains = [gain_ref[:, p * span : (p + 1) * span].astype(jnp.float32) for p in range(parts)]
    block, tags = kept_ref[...].astype(jnp.float32), tags_ref[...].astype(jnp.float32)
    for at, _, height in regions(base_ref.shape[0] // parts, parts):
        pieces = [block[at + p * height : at + (p + 1) * height] for p in range(parts)]
        ids = tags[at : at + height]
        scale = lax.rsqrt(spread_of(pieces) + 1e-06)
        normed = [(v * scale * gain).astype(jnp.bfloat16) for v, gain in zip(pieces, gains)]
        logits = sum(across(v, router_ref[:, p * span : (p + 1) * span]) for p, v in enumerate(normed))
        gates = sigmoid(logits)
        id_range = lax.broadcasted_iota(jnp.int32, gates.shape, 1)
        named = id_range.astype(jnp.float32)
        picked = sum((ids[:, k : k + 1] == named).astype(jnp.float32) for k in range(top_count))
        share = jnp.sum(jnp.where(id_range >= n_real, picked * gates, 0.0), axis=-1, keepdims=True)
        for p in range(parts):
            rows = slice(at + p * height, at + (p + 1) * height)
            base_ref[rows, :] = pieces[p] + share * normed[p].astype(jnp.float32)


def layer_kernel(rows, parts, place_ref, all_ref, gain_ref, router_ref, *refs):
    tags_ref = None
    if len(refs) > REFS:
        tags_ref, *refs = refs
    sources, out_ref = refs[:6], refs[6]
    held = refs[7:13]
    d_down, e_down = held[2], held[5]
    normed_ref, coef_ref, d_hidden, e_hidden, value_ref, stage_ref, sems, out_sems = refs[13:]
    n_groups = all_ref.shape[0]
    span = out_ref.shape[2]
    width = parts * span
    place = place_ref[0]
    unit = 16 // math.gcd(rows, 16)
    unit = unit if n_groups % unit == 0 else n_groups

    out_cuts = column_cuts(span, OUT)
    if span % OUT == 0 and OUT % (2 * LANES) == 0:
        out_cuts = out_cuts[:-1] + [(span - OUT, OUT // 2), (span - OUT // 2, OUT // 2)]
    plan = []
    for which, hidden_ref in ((0, d_hidden), (3, e_hidden)):
        joined = hidden_ref.shape[1] % LANES == 0
        for at, size in column_cuts(hidden_ref.shape[1], HIDDEN):
            spots = (2 * at, 2 * at + size) if joined else (at, at)
            plan += [(which, at, spots[0], size), (which + 1, at, spots[1], size)]
    for at, size in out_cuts:
        plan += [(which, p * span + at, p * span + at, size) for which in (2, 5) for p in range(parts)]
    held = tuple(
        held[i - 1] if i in (1, 4) and refs_joined(held[i - 1], sources[i]) else h for i, h in enumerate(held)
    )
    order, owned, volume, total = [], {}, [], 0
    for which, at, put, size in plan:
        height = held[which].shape[0]
        pieces = max(1, height * size * 2 // PIECE)
        pieces = pieces if height % pieces == 0 and height // pieces % 16 == 0 else 1
        owned[which, at] = range(len(order), len(order) + pieces)
        for k in range(pieces):
            lines = pl.ds(k * (height // pieces), height // pieces)
            source, target = sources[which].at[lines, pl.ds(at, size)], held[which].at[lines, pl.ds(put, size)]
            order.append(pltpu.make_async_copy(source, target, sems.at[len(order)]))
            total += height // pieces * size * 2
            volume.append(total)
    begun = [0]

    def start_until(limit):
        while begun[0] < len(order) and volume[begun[0]] <= limit:
            order[begun[0]].start()
            begun[0] += 1

    start_until(max(FLIGHT, volume[0]))

    def arrive(which, at):
        for i in owned[which, at]:
            order[i].wait()
            start_until(volume[i] + FLIGHT)

    def load(step, carry):
        blocks = [all_ref[step * unit + u].astype(jnp.float32) for u in range(unit)]
        if tags_ref is None:
            tags = [b[:, span:] for b in blocks]
        else:
            tags = [tags_ref[step * unit + u].astype(jnp.float32) for u in range(unit)]
        for at, first, height in regions(rows, parts):
            start = pl.multiple_of(n_groups * first + step * unit * height, 16)
            here = pl.ds(start, unit * height)
            pieces = [
                jnp.concatenate([b[at + p * height : at + (p + 1) * height, :span] for b in blocks], axis=0)
                for p in range(parts)
            ]
            ids = jnp.concatenate([t[at : at + height] for t in tags], axis=0)
            named = jnp.sum((ids == place.astype(jnp.float32)).astype(jnp.float32), axis=-1, keepdims=True)
            scale = lax.rsqrt(spread_of(pieces) + 1e-06)
            for p, v in enumerate(pieces):
                gain = gain_ref[:, p * span : (p + 1) * span].astype(jnp.float32)
                normed_ref[here, p * span : (p + 1) * span] = (v * scale * gain).astype(jnp.bfloat16)
            coef_ref[here, :] = jnp.broadcast_to(named, (unit * height, LANES))
        return carry

    lax.fori_loop(0, n_groups // unit, load, 0)

    logits = across(normed_ref[...], router_ref[...])
    mine = lax.broadcasted_iota(jnp.int32, logits.shape, 1) == place
    gate = jnp.sum(jnp.where(mine, sigmoid(logits), 0.0), axis=-1, keepdims=True)
    coef_ref[...] = coef_ref[...] * gate

    def hidden(which, target):
        joined = target.shape[1] % LANES == 0
        for at, size in column_cuts(target.shape[1], HIDDEN):
            arrive(which, at)
            arrive(which + 1, at)
            if joined:
                pair = jnp.dot(
                    normed_ref[...], held[which][:, 2 * at : 2 * (at + size)], preferred_element_type=jnp.float32
                )
                gate_part, up_part = pair[:, :size], pair[:, size:]
            else:
                gate_part, up_part = (
                    jnp.dot(normed_ref[...], held[w][:, at : at + size], preferred_element_type=jnp.float32)
                    for w in (which, which + 1)
                )
            target[:, at : at + size] = (gate_part * sigmoid(gate_part) * up_part).astype(jnp.bfloat16)

    hidden(0, d_hidden)
    hidden(3, e_hidden)

    leaving = []
    for at, size in out_cuts:
        for which in (2, 5):
            for p in range(parts):
                arrive(which, p * span + at)
        for p in range(parts):
            cols = slice(p * span + at, p * span + at + size)
            dense = jnp.dot(d_hidden[...], d_down[:, cols], preferred_element_type=jnp.float32)
            routed = jnp.dot(e_hidden[...], e_down[:, cols], preferred_element_type=jnp.float32)
            value_ref[:, p * OUT : p * OUT + size] = dense + coef_ref[:, :1] * routed

        def pack(step, carry):
            rows_of = []
            for _, first, height in regions(rows, parts):
                start = pl.multiple_of(n_groups * first + step * unit * height, SUBLANES)
                rows_of.append((height, value_ref[pl.ds(start, unit * height), :]))
            for u in range(unit):
                pieces = [
                    tall[u * height : (u + 1) * height, p * OUT : p * OUT + size]
                    for height, tall in rows_of
                    for p in range(parts)
                ]
                block = jnp.concatenate(pieces, axis=0).astype(out_ref.dtype)
                stage_ref[step * unit + u, :, at : at + size] = block
            return carry

        lax.fori_loop(0, n_groups // unit, pack, 0)
        cols = pl.ds(at, size)
        leaving.append(pltpu.make_async_copy(stage_ref.at[:, :, cols], out_ref.at[:, :, cols], out_sems.at[len(leaving)]))
        leaving[-1].start()
    for copy in leaving:
        copy.wait()


def combine_kernel(parts, got_ref, base_ref, folded_ref, flat_ref, total_ref):
    per_group, n_micro, width = flat_ref.shape
    rows, span = n_micro * per_group, base_ref.shape[1]
    total = base_ref[...]
    for g in range(got_ref.shape[0]):
        total = total + got_ref[g].astype(jnp.float32)
    folded_ref[...] = total.astype(jnp.bfloat16)
    total_ref[...] = total
    step = math.gcd(n_micro, SUBLANES)
    for i in range(per_group):
        for m in range(0, n_micro, step):
            for p in range(parts):
                at = place_in_block(rows, parts, p, i * n_micro + m)
                cols = slice(p * span, (p + 1) * span)
                flat_ref[i, m : m + step, cols] = total_ref[at : at + step, :].astype(jnp.bfloat16)


def layer(fed, ids, known, gain, router_t, weights, parts):
    per_group, n_micro, top_count = ids.shape
    n_groups = lax.axis_size("ep")
    n_pairs = lax.axis_size("tp")
    place = lax.axis_index("ep")
    width = gain.shape[1]
    rows, span = n_micro * per_group, width // parts
    tall, wide = parts * rows, span + LANES
    count = n_groups * rows

    params = pltpu.CompilerParams(vmem_limit_bytes=16 * MIB)
    if known is None:
        sent, kept, tags = pl.pallas_call(
            lambda *refs: first_pack_kernel(parts, *refs),
            out_shape=[
                jax.ShapeDtypeStruct((n_groups, tall, wide), jnp.bfloat16),
                jax.ShapeDtypeStruct((tall, span), jnp.bfloat16),
                jax.ShapeDtypeStruct((tall, LANES), jnp.bfloat16),
            ],
            in_specs=[OUTSIDE, OUTSIDE],
            out_specs=[WHOLE] * 3,
            scratch_shapes=[
                pltpu.VMEM(fed.shape, fed.dtype),
                pltpu.VMEM(ids.shape, ids.dtype),
                pltpu.VMEM((tall, LANES), jnp.float32),
                pltpu.VMEM((tall, span), jnp.float32),
                pltpu.SemaphoreType.DMA((2,)),
            ],
            compiler_params=params,
            name="pack",
        )(fed, ids)
        all_tags = []
    else:
        kept, tags, all_tags = fed, known[0], [known[1]]
        sent = pl.pallas_call(
            later_pack_kernel,
            out_shape=jax.ShapeDtypeStruct((n_groups, tall, span), jnp.bfloat16),
            in_specs=[WHOLE],
            out_specs=WHOLE,
            compiler_params=params,
            name="pack",
        )(fed)
    gathered = exchange(sent, "ep")

    blank_groups = n_groups if known is None else 1
    base, blank = pl.pallas_call(
        lambda *refs: base_kernel(n_groups, top_count, parts, *refs),
        out_shape=[
            jax.ShapeDtypeStruct((tall, span), jnp.float32),
            jax.ShapeDtypeStruct((blank_groups, tall, LANES), jnp.bfloat16),
        ],
        in_specs=[WHOLE] * 4,
        out_specs=[WHOLE, WHOLE],
        compiler_params=pltpu.CompilerParams(vmem_limit_bytes=8 * MIB),
        cost_estimate=pl.CostEstimate(flops=int(1e8), bytes_accessed=int(1e6), transcendentals=0),
        name="base",
    )(kept, tags, gain, router_t)

    n_dense, n_expert = weights[0].shape[1], weights[3].shape[1]
    weights = [pltpu.with_memory_space_constraint(w, pltpu.HBM) for w in weights]
    partial = pl.pallas_call(
        lambda *refs: layer_kernel(rows, parts, *refs),
        out_shape=jax.ShapeDtypeStruct((n_groups, tall, span), jnp.bfloat16),
        in_specs=[SCALAR] + [WHOLE] * (3 + len(all_tags)) + [pl.BlockSpec(memory_space=pltpu.HBM)] * 6,
        out_specs=OUTSIDE,
        scratch_shapes=[
            *(pltpu.VMEM(shape, jnp.bfloat16) for shape in pair_shapes(width, n_dense)),
            pltpu.VMEM((n_dense, width), jnp.bfloat16),
            *(pltpu.VMEM(shape, jnp.bfloat16) for shape in pair_shapes(width, n_expert)),
            pltpu.VMEM((n_expert, width), jnp.bfloat16),
            pltpu.VMEM((count, width), jnp.bfloat16),
            pltpu.VMEM((count, LANES), jnp.float32),
            pltpu.VMEM((count, n_dense), jnp.bfloat16),
            pltpu.VMEM((count, n_expert), jnp.bfloat16),
            pltpu.VMEM((count, parts * OUT), jnp.float32),
            pltpu.VMEM((n_groups, tall, span), jnp.bfloat16),
            pltpu.SemaphoreType.DMA((128,)),
            pltpu.SemaphoreType.DMA((16,)),
        ],
        compiler_params=pltpu.CompilerParams(vmem_limit_bytes=50 * MIB),
        cost_estimate=pl.CostEstimate(
            flops=6 * count * width * (n_dense + n_expert),
            bytes_accessed=6 * width * (n_dense + n_expert),
            transcendentals=0,
        ),
        name="layer",
    )(place.reshape(1).astype(jnp.int32), gathered, gain, router_t, *all_tags, *weights)

    share = tall // n_pairs
    received = exchange(partial.reshape(n_groups * n_pairs, share, span), ("ep", "tp"))
    if n_pairs > 1:
        kept_base = lax.dynamic_slice_in_dim(base, lax.axis_index("tp") * share, share, 0)
        part = (kept_base + jnp.sum(received.astype(jnp.float32), axis=0)).astype(jnp.bfloat16)
        folded = lax.all_gather(part, "tp", axis=0, tiled=True)
        return folded, unfold(folded, parts).reshape(per_group, n_micro, width), blank
    folded, flat = pl.pallas_call(
        lambda *refs: combine_kernel(parts, *refs),
        out_shape=[
            jax.ShapeDtypeStruct((tall, span), jnp.bfloat16),
            jax.ShapeDtypeStruct((per_group, n_micro, width), jnp.bfloat16),
        ],
        in_specs=[WHOLE, WHOLE],
        out_specs=[WHOLE, WHOLE],
        scratch_shapes=[pltpu.VMEM((tall, span), jnp.float32)],
        compiler_params=pltpu.CompilerParams(vmem_limit_bytes=8 * MIB),
        name="combine",
    )(received, base)
    return folded, flat, blank


def early_tags(ids, parts):
    per_group, n_micro, _ = ids.shape
    n_groups, tall = lax.axis_size("ep"), parts * per_group * n_micro
    sent, tags = pl.pallas_call(
        lambda *refs: tags_kernel(parts, *refs),
        out_shape=[
            jax.ShapeDtypeStruct((n_groups, tall, LANES), jnp.bfloat16),
            jax.ShapeDtypeStruct((tall, LANES), jnp.bfloat16),
        ],
        in_specs=[WHOLE],
        out_specs=[WHOLE, WHOLE],
        scratch_shapes=[pltpu.VMEM((tall, LANES), jnp.float32)],
        compiler_params=pltpu.CompilerParams(vmem_limit_bytes=8 * MIB),
        name="tags",
    )(ids)
    settled = pl.pallas_call(
        settle_kernel,
        out_shape=pltpu.HBM(sent.shape, sent.dtype),
        in_specs=[WHOLE],
        out_specs=pl.BlockSpec(memory_space=pltpu.HBM),
        scratch_shapes=[pltpu.SemaphoreType.DMA],
        compiler_params=pltpu.CompilerParams(vmem_limit_bytes=8 * MIB),
        name="settle",
    )(exchange(sent, "ep"))
    return tags, settled


def on_device(
    acts,
    route_ids,
    norm_gain,
    router,
    dense_gate,
    dense_up,
    dense_down,
    expert_gate,
    expert_up,
    expert_down,
):
    n_micro, per_group, width = acts.shape
    n_sections = lax.axis_size("pp")
    section = lax.axis_index("pp")
    rows = n_micro * per_group
    parts = SUBLANES // math.gcd(rows, SUBLANES)
    weights = (
        dense_gate[0],
        dense_up[0],
        dense_down[0],
        expert_gate[0, 0],
        expert_up[0, 0],
        expert_down[0, 0],
    )
    router_t = router[0].T

    fed = acts.swapaxes(0, 1)
    ids = route_ids[0].swapaxes(0, 1)
    n_groups = lax.axis_size("ep")
    tall = parts * rows

    def first(given):
        folded, flat, blank = layer(given, ids, None, norm_gain, router_t, weights, parts)
        return folded, flat, jnp.zeros((tall, LANES), jnp.bfloat16), blank

    def idle(given):
        folded = jnp.zeros((tall, width // parts), jnp.bfloat16)
        return folded, jnp.zeros((per_group, n_micro, width), jnp.bfloat16), *early_tags(ids, parts)

    folded, flat, *known = lax.cond(section == 0, first, idle, fed)
    for phase in range(1, n_sections):
        fed = lax.ppermute(folded, "pp", [(phase - 1, phase)])
        folded, flat = lax.cond(
            section == phase,
            lambda held, given: layer(given, ids, known, norm_gain, router_t, weights, parts)[:2],
            lambda held, given: held,
            (folded, flat),
            fed,
        )
    return flat.swapaxes(0, 1)[None]


def solution(mesh):
    return jax.shard_map(
        on_device,
        mesh=mesh,
        in_specs=(
            P(None, "ep", None),
            P("pp", None, "ep", None),
            P("pp", None),
            P("pp", None, None),
            P("pp", None, ("ep", "tp")),
            P("pp", None, ("ep", "tp")),
            P("pp", ("ep", "tp"), None),
            P("pp", "ep", None, "tp"),
            P("pp", "ep", None, "tp"),
            P("pp", "ep", "tp", None),
        ),
        out_specs=P("pp", None, "ep", None),
        check_vma=False,
    )
```

```python
import math

import jax
import jax.numpy as jnp
from jax import lax
from jax.experimental import pallas as pl
from jax.experimental.pallas import tpu as pltpu
from jax.sharding import PartitionSpec as P

LANES = 128
SUBLANES = 8
MIB = 1 << 20
FLIGHT = 12 * MIB
PIECE = 3 * MIB // 4
HIDDEN = 256
OUT = 512
WHOLE = pl.BlockSpec(memory_space=pltpu.VMEM)
SCALAR = pl.BlockSpec(memory_space=pltpu.SMEM)
OUTSIDE = pl.BlockSpec(memory_space=pl.ANY)


def exchange(blocks, axes):
    return lax.all_to_all(blocks, axes, split_axis=0, concat_axis=0, tiled=True)


def unfold(folded, parts):
    tall = folded.shape[0]
    lines = []
    for at, _, height in regions(tall // parts, parts):
        pieces = [folded[at + p * height : at + (p + 1) * height] for p in range(parts)]
        lines.append(jnp.concatenate(pieces, axis=1))
    return jnp.concatenate(lines, axis=0)


def sigmoid(v):
    return 1.0 / (1.0 + jnp.exp(-v))


def across(a, b):
    return lax.dot_general(a, b, (((1,), (1,)), ((), ())), preferred_element_type=jnp.float32)


def spread_of(pieces):
    count = sum(v.shape[1] for v in pieces)
    return sum(jnp.sum(v * v, axis=-1, keepdims=True) for v in pieces) / count


def regions(rows, parts):
    even = rows // SUBLANES * SUBLANES
    found = [(0, 0, even), (parts * even, even, rows - even)]
    return [region for region in found if region[2] > 0]


def place_in_block(rows, parts, part, row):
    for at, first, height in regions(rows, parts):
        if first <= row < first + height:
            return at + part * height + row - first


def pair_shapes(width, count):
    if count % LANES == 0:
        return [(width, 2 * count), (SUBLANES, LANES)]
    return [(width, count)] * 2


def refs_joined(held, source):
    return held.shape[1] == 2 * source.shape[1]


def column_cuts(total, size):
    return [(at, min(size, total - at)) for at in range(0, total, size)]


def write_tags(ids_ref, rows, parts, tags_ref):
    per_group, n_micro, top_count = ids_ref.shape
    step = math.gcd(n_micro, SUBLANES)
    tags_ref[...] = jnp.full(tags_ref.shape, -1.0, jnp.float32)
    for i in range(per_group):
        ids = ids_ref[i].astype(jnp.float32)
        for m in range(0, n_micro, step):
            at = place_in_block(rows, parts, 0, i * n_micro + m)
            tags_ref[at : at + step, :top_count] = ids[m : m + step]


def tags_kernel(parts, ids_ref, sent_ref, kept_ref, tags_ref):
    write_tags(ids_ref, tags_ref.shape[0] // parts, parts, tags_ref)
    block = tags_ref[...].astype(jnp.bfloat16)
    kept_ref[...] = block
    for g in range(sent_ref.shape[0]):
        sent_ref[g] = block


def settle_kernel(tags_ref, out_ref, sem):
    copy = pltpu.make_async_copy(tags_ref, out_ref, sem)
    copy.start()
    copy.wait()


def first_pack_kernel(parts, x_hbm, ids_hbm, sent_ref, kept_ref, kept_tags_ref, x_ref, ids_ref, tags_ref, block_ref, sems):
    copies = [
        pltpu.make_async_copy(x_hbm, x_ref, sems.at[0]),
        pltpu.make_async_copy(ids_hbm, ids_ref, sems.at[1]),
    ]
    for copy in copies:
        copy.start()
    for copy in copies:
        copy.wait()
    per_group, n_micro, _ = x_ref.shape
    rows, span = per_group * n_micro, block_ref.shape[1]
    step = math.gcd(n_micro, SUBLANES)
    write_tags(ids_ref, rows, parts, tags_ref)
    for i in range(per_group):
        mine = x_ref[i].astype(jnp.float32)
        for m in range(0, n_micro, step):
            for p in range(parts):
                at = place_in_block(rows, parts, p, i * n_micro + m)
                block_ref[at : at + step, :] = mine[m : m + step, p * span : (p + 1) * span]
    block, tags = block_ref[...].astype(jnp.bfloat16), tags_ref[...].astype(jnp.bfloat16)
    kept_ref[...] = block
    kept_tags_ref[...] = tags
    for g in range(sent_ref.shape[0]):
        sent_ref[g, :, :span] = block
        sent_ref[g, :, span:] = tags


def later_pack_kernel(x_ref, sent_ref):
    for g in range(sent_ref.shape[0]):
        sent_ref[g] = x_ref[...]


def base_kernel(n_real, top_count, parts, kept_ref, tags_ref, gain_ref, router_ref, base_ref, blank_ref):
    blank_ref[...] = jnp.zeros(blank_ref.shape, blank_ref.dtype)
    span = base_ref.shape[1]
    gains = [gain_ref[:, p * span : (p + 1) * span].astype(jnp.float32) for p in range(parts)]
    block, tags = kept_ref[...].astype(jnp.float32), tags_ref[...].astype(jnp.float32)
    for at, _, height in regions(base_ref.shape[0] // parts, parts):
        pieces = [block[at + p * height : at + (p + 1) * height] for p in range(parts)]
        ids = tags[at : at + height]
        scale = lax.rsqrt(spread_of(pieces) + 1e-06)
        normed = [(v * scale * gain).astype(jnp.bfloat16) for v, gain in zip(pieces, gains)]
        logits = sum(across(v, router_ref[:, p * span : (p + 1) * span]) for p, v in enumerate(normed))
        gates = sigmoid(logits)
        id_range = lax.broadcasted_iota(jnp.int32, gates.shape, 1)
        named = id_range.astype(jnp.float32)
        picked = sum((ids[:, k : k + 1] == named).astype(jnp.float32) for k in range(top_count))
        share = jnp.sum(jnp.where(id_range >= n_real, picked * gates, 0.0), axis=-1, keepdims=True)
        for p in range(parts):
            rows = slice(at + p * height, at + (p + 1) * height)
            base_ref[rows, :] = pieces[p] + share * normed[p].astype(jnp.float32)


def head_kernel(gate_ref, up_ref, head_ref, sems):
    size = head_ref.shape[1] // 2
    cols = pl.ds(gate_ref.shape[1] - size, size)
    copies = [
        pltpu.make_async_copy(source.at[:, cols], head_ref.at[:, pl.ds(i * size, size)], sems.at[i])
        for i, source in enumerate((gate_ref, up_ref))
    ]
    for copy in copies:
        copy.start()
    for copy in copies:
        copy.wait()


def layer_kernel(rows, parts, tagged, headed, place_ref, all_ref, gain_ref, router_ref, *refs):
    tags_ref, head_ref = None, None
    if not tagged:
        tags_ref, *refs = refs
    if headed:
        head_ref, *refs = refs
    early = head_ref.shape[1] // 2 if headed else 0
    sources, out_ref = refs[:6], refs[6]
    held = refs[7:13]
    d_down, e_down = held[2], held[5]
    normed_ref, coef_ref, d_hidden, e_hidden, value_ref, stage_ref, sems, out_sems = refs[13:]
    n_groups = all_ref.shape[0]
    span = out_ref.shape[2]
    width = parts * span
    place = place_ref[0]
    unit = 16 // math.gcd(rows, 16)
    unit = unit if n_groups % unit == 0 else n_groups

    out_cuts = column_cuts(span, OUT)
    if span % OUT == 0 and OUT % (2 * LANES) == 0:
        out_cuts = out_cuts[:-1] + [(span - OUT, OUT // 2), (span - OUT // 2, OUT // 2)]
    plan = []
    for which, hidden_ref in ((0, d_hidden), (3, e_hidden)):
        joined = hidden_ref.shape[1] % LANES == 0
        streamed = hidden_ref.shape[1] - (early if which == 0 else 0)
        for at, size in column_cuts(streamed, HIDDEN):
            spots = (2 * at, 2 * at + size) if joined else (at, at)
            plan += [(which, at, spots[0], size), (which + 1, at, spots[1], size)]
    for at, size in out_cuts:
        plan += [(which, p * span + at, p * span + at, size) for which in (2, 5) for p in range(parts)]
    held = tuple(
        held[i - 1] if i in (1, 4) and refs_joined(held[i - 1], sources[i]) else h for i, h in enumerate(held)
    )
    order, owned, volume, total = [], {}, [], 0
    for which, at, put, size in plan:
        height = held[which].shape[0]
        pieces = max(1, height * size * 2 // PIECE)
        pieces = pieces if height % pieces == 0 and height // pieces % 16 == 0 else 1
        owned[which, at] = range(len(order), len(order) + pieces)
        for k in range(pieces):
            lines = pl.ds(k * (height // pieces), height // pieces)
            source, target = sources[which].at[lines, pl.ds(at, size)], held[which].at[lines, pl.ds(put, size)]
            order.append(pltpu.make_async_copy(source, target, sems.at[len(order)]))
            total += height // pieces * size * 2
            volume.append(total)
    begun = [0]

    def start_until(limit):
        while begun[0] < len(order) and volume[begun[0]] <= limit:
            order[begun[0]].start()
            begun[0] += 1

    start_until(max(FLIGHT, volume[0]))

    def arrive(which, at):
        for i in owned[which, at]:
            order[i].wait()
            start_until(volume[i] + FLIGHT)

    def load(step, carry):
        blocks = [all_ref[step * unit + u].astype(jnp.float32) for u in range(unit)]
        if tags_ref is None:
            tags = [b[:, span:] for b in blocks]
        else:
            tags = [tags_ref[step * unit + u].astype(jnp.float32) for u in range(unit)]
        for at, first, height in regions(rows, parts):
            start = pl.multiple_of(n_groups * first + step * unit * height, 16)
            here = pl.ds(start, unit * height)
            pieces = [
                jnp.concatenate([b[at + p * height : at + (p + 1) * height, :span] for b in blocks], axis=0)
                for p in range(parts)
            ]
            ids = jnp.concatenate([t[at : at + height] for t in tags], axis=0)
            named = jnp.sum((ids == place.astype(jnp.float32)).astype(jnp.float32), axis=-1, keepdims=True)
            scale = lax.rsqrt(spread_of(pieces) + 1e-06)
            for p, v in enumerate(pieces):
                gain = gain_ref[:, p * span : (p + 1) * span].astype(jnp.float32)
                normed_ref[here, p * span : (p + 1) * span] = (v * scale * gain).astype(jnp.bfloat16)
            coef_ref[here, :] = jnp.broadcast_to(named, (unit * height, LANES))
        return carry

    lax.fori_loop(0, n_groups // unit, load, 0)

    logits = across(normed_ref[...], router_ref[...])
    mine = lax.broadcasted_iota(jnp.int32, logits.shape, 1) == place
    gate = jnp.sum(jnp.where(mine, sigmoid(logits), 0.0), axis=-1, keepdims=True)
    coef_ref[...] = coef_ref[...] * gate

    def hidden(which, target):
        joined = target.shape[1] % LANES == 0
        streamed = target.shape[1]
        if which == 0 and headed:
            streamed -= early
            pair = jnp.dot(normed_ref[...], head_ref[...], preferred_element_type=jnp.float32)
            gate_part, up_part = pair[:, :early], pair[:, early:]
            target[:, streamed:] = (gate_part * sigmoid(gate_part) * up_part).astype(jnp.bfloat16)
        for at, size in column_cuts(streamed, HIDDEN):
            arrive(which, at)
            arrive(which + 1, at)
            if joined:
                pair = jnp.dot(
                    normed_ref[...], held[which][:, 2 * at : 2 * (at + size)], preferred_element_type=jnp.float32
                )
                gate_part, up_part = pair[:, :size], pair[:, size:]
            else:
                gate_part, up_part = (
                    jnp.dot(normed_ref[...], held[w][:, at : at + size], preferred_element_type=jnp.float32)
                    for w in (which, which + 1)
                )
            target[:, at : at + size] = (gate_part * sigmoid(gate_part) * up_part).astype(jnp.bfloat16)

    hidden(0, d_hidden)
    hidden(3, e_hidden)

    leaving = []
    for at, size in out_cuts:
        for which in (2, 5):
            for p in range(parts):
                arrive(which, p * span + at)
        for p in range(parts):
            cols = slice(p * span + at, p * span + at + size)
            dense = jnp.dot(d_hidden[...], d_down[:, cols], preferred_element_type=jnp.float32)
            routed = jnp.dot(e_hidden[...], e_down[:, cols], preferred_element_type=jnp.float32)
            value_ref[:, p * OUT : p * OUT + size] = dense + coef_ref[:, :1] * routed

        def pack(step, carry):
            rows_of = []
            for _, first, height in regions(rows, parts):
                start = pl.multiple_of(n_groups * first + step * unit * height, SUBLANES)
                rows_of.append((height, value_ref[pl.ds(start, unit * height), :]))
            for u in range(unit):
                pieces = [
                    tall[u * height : (u + 1) * height, p * OUT : p * OUT + size]
                    for height, tall in rows_of
                    for p in range(parts)
                ]
                block = jnp.concatenate(pieces, axis=0).astype(out_ref.dtype)
                stage_ref[step * unit + u, :, at : at + size] = block
            return carry

        lax.fori_loop(0, n_groups // unit, pack, 0)
        cols = pl.ds(at, size)
        leaving.append(pltpu.make_async_copy(stage_ref.at[:, :, cols], out_ref.at[:, :, cols], out_sems.at[len(leaving)]))
        leaving[-1].start()
    for copy in leaving:
        copy.wait()


def combine_kernel(parts, got_ref, base_ref, folded_ref, flat_ref, total_ref):
    per_group, n_micro, width = flat_ref.shape
    rows, span = n_micro * per_group, base_ref.shape[1]
    total = base_ref[...]
    for g in range(got_ref.shape[0]):
        total = total + got_ref[g].astype(jnp.float32)
    folded_ref[...] = total.astype(jnp.bfloat16)
    total_ref[...] = total
    step = math.gcd(n_micro, SUBLANES)
    for i in range(per_group):
        for m in range(0, n_micro, step):
            for p in range(parts):
                at = place_in_block(rows, parts, p, i * n_micro + m)
                cols = slice(p * span, (p + 1) * span)
                flat_ref[i, m : m + step, cols] = total_ref[at : at + step, :].astype(jnp.bfloat16)


def layer(fed, ids, known, gain, router_t, weights, parts):
    per_group, n_micro, top_count = ids.shape
    n_groups = lax.axis_size("ep")
    n_pairs = lax.axis_size("tp")
    place = lax.axis_index("ep")
    width = gain.shape[1]
    rows, span = n_micro * per_group, width // parts
    tall, wide = parts * rows, span + LANES
    count = n_groups * rows

    params = pltpu.CompilerParams(vmem_limit_bytes=16 * MIB)
    if known is None:
        sent, kept, tags = pl.pallas_call(
            lambda *refs: first_pack_kernel(parts, *refs),
            out_shape=[
                jax.ShapeDtypeStruct((n_groups, tall, wide), jnp.bfloat16),
                jax.ShapeDtypeStruct((tall, span), jnp.bfloat16),
                jax.ShapeDtypeStruct((tall, LANES), jnp.bfloat16),
            ],
            in_specs=[OUTSIDE, OUTSIDE],
            out_specs=[WHOLE] * 3,
            scratch_shapes=[
                pltpu.VMEM(fed.shape, fed.dtype),
                pltpu.VMEM(ids.shape, ids.dtype),
                pltpu.VMEM((tall, LANES), jnp.float32),
                pltpu.VMEM((tall, span), jnp.float32),
                pltpu.SemaphoreType.DMA((2,)),
            ],
            compiler_params=params,
            name="pack",
        )(fed, ids)
        all_tags = []
    else:
        kept, tags, all_tags = fed, known[0], [known[1]]
        sent = pl.pallas_call(
            later_pack_kernel,
            out_shape=jax.ShapeDtypeStruct((n_groups, tall, span), jnp.bfloat16),
            in_specs=[WHOLE],
            out_specs=WHOLE,
            compiler_params=params,
            name="pack",
        )(fed)
    gathered = exchange(sent, "ep")

    blank_groups = n_groups if known is None else 1
    base, blank = pl.pallas_call(
        lambda *refs: base_kernel(n_groups, top_count, parts, *refs),
        out_shape=[
            jax.ShapeDtypeStruct((tall, span), jnp.float32),
            jax.ShapeDtypeStruct((blank_groups, tall, LANES), jnp.bfloat16),
        ],
        in_specs=[WHOLE] * 4,
        out_specs=[WHOLE, WHOLE],
        compiler_params=pltpu.CompilerParams(vmem_limit_bytes=8 * MIB),
        cost_estimate=pl.CostEstimate(flops=int(1e8), bytes_accessed=int(1e6), transcendentals=0),
        name="base",
    )(kept, tags, gain, router_t)

    n_dense, n_expert = weights[0].shape[1], weights[3].shape[1]
    early = n_dense % HIDDEN if n_dense > HIDDEN and n_dense % LANES == 0 else 0
    heads = []
    if early:
        head = pl.pallas_call(
            head_kernel,
            out_shape=pltpu.VMEM((width, 2 * early), jnp.bfloat16),
            in_specs=[pl.BlockSpec(memory_space=pltpu.HBM)] * 2,
            out_specs=WHOLE,
            scratch_shapes=[pltpu.SemaphoreType.DMA((2,))],
            compiler_params=pltpu.CompilerParams(vmem_limit_bytes=4 * MIB),
            cost_estimate=pl.CostEstimate(flops=int(1e9), bytes_accessed=early * width * 4, transcendentals=0),
            name="head",
        )(*(pltpu.with_memory_space_constraint(w, pltpu.HBM) for w in weights[:2]))
        heads = [pltpu.with_memory_space_constraint(head, pltpu.VMEM)]
    weights = [pltpu.with_memory_space_constraint(w, pltpu.HBM) for w in weights]
    partial = pl.pallas_call(
        lambda *refs: layer_kernel(rows, parts, known is None, early > 0, *refs),
        out_shape=pltpu.HBM((n_groups, tall, span), jnp.bfloat16),
        in_specs=[SCALAR] + [WHOLE] * (3 + len(all_tags) + len(heads)) + [pl.BlockSpec(memory_space=pltpu.HBM)] * 6,
        out_specs=pl.BlockSpec(memory_space=pltpu.HBM),
        scratch_shapes=[
            *(pltpu.VMEM(shape, jnp.bfloat16) for shape in pair_shapes(width, n_dense)),
            pltpu.VMEM((n_dense, width), jnp.bfloat16),
            *(pltpu.VMEM(shape, jnp.bfloat16) for shape in pair_shapes(width, n_expert)),
            pltpu.VMEM((n_expert, width), jnp.bfloat16),
            pltpu.VMEM((count, width), jnp.bfloat16),
            pltpu.VMEM((count, LANES), jnp.float32),
            pltpu.VMEM((count, n_dense), jnp.bfloat16),
            pltpu.VMEM((count, n_expert), jnp.bfloat16),
            pltpu.VMEM((count, parts * OUT), jnp.float32),
            pltpu.VMEM((n_groups, tall, span), jnp.bfloat16),
            pltpu.SemaphoreType.DMA((128,)),
            pltpu.SemaphoreType.DMA((16,)),
        ],
        compiler_params=pltpu.CompilerParams(vmem_limit_bytes=50 * MIB),
        cost_estimate=pl.CostEstimate(
            flops=6 * count * width * (n_dense + n_expert),
            bytes_accessed=6 * width * (n_dense + n_expert),
            transcendentals=0,
        ),
        name="layer",
    )(place.reshape(1).astype(jnp.int32), gathered, gain, router_t, *all_tags, *heads, *weights)

    share = tall // n_pairs
    received = exchange(partial.reshape(n_groups * n_pairs, share, span), ("ep", "tp"))
    if n_pairs > 1:
        kept_base = lax.dynamic_slice_in_dim(base, lax.axis_index("tp") * share, share, 0)
        part = (kept_base + jnp.sum(received.astype(jnp.float32), axis=0)).astype(jnp.bfloat16)
        folded = lax.all_gather(part, "tp", axis=0, tiled=True)
        return folded, unfold(folded, parts).reshape(per_group, n_micro, width), blank
    folded, flat = pl.pallas_call(
        lambda *refs: combine_kernel(parts, *refs),
        out_shape=[
            jax.ShapeDtypeStruct((tall, span), jnp.bfloat16),
            jax.ShapeDtypeStruct((per_group, n_micro, width), jnp.bfloat16),
        ],
        in_specs=[WHOLE, WHOLE],
        out_specs=[WHOLE, WHOLE],
        scratch_shapes=[pltpu.VMEM((tall, span), jnp.float32)],
        compiler_params=pltpu.CompilerParams(vmem_limit_bytes=8 * MIB),
        name="combine",
    )(received, base)
    return folded, flat, blank


def early_tags(ids, parts):
    per_group, n_micro, _ = ids.shape
    n_groups, tall = lax.axis_size("ep"), parts * per_group * n_micro
    sent, tags = pl.pallas_call(
        lambda *refs: tags_kernel(parts, *refs),
        out_shape=[
            jax.ShapeDtypeStruct((n_groups, tall, LANES), jnp.bfloat16),
            jax.ShapeDtypeStruct((tall, LANES), jnp.bfloat16),
        ],
        in_specs=[WHOLE],
        out_specs=[WHOLE, WHOLE],
        scratch_shapes=[pltpu.VMEM((tall, LANES), jnp.float32)],
        compiler_params=pltpu.CompilerParams(vmem_limit_bytes=8 * MIB),
        name="tags",
    )(ids)
    settled = pl.pallas_call(
        settle_kernel,
        out_shape=pltpu.HBM(sent.shape, sent.dtype),
        in_specs=[WHOLE],
        out_specs=pl.BlockSpec(memory_space=pltpu.HBM),
        scratch_shapes=[pltpu.SemaphoreType.DMA],
        compiler_params=pltpu.CompilerParams(vmem_limit_bytes=8 * MIB),
        name="settle",
    )(exchange(sent, "ep"))
    return tags, settled


def on_device(
    acts,
    route_ids,
    norm_gain,
    router,
    dense_gate,
    dense_up,
    dense_down,
    expert_gate,
    expert_up,
    expert_down,
):
    n_micro, per_group, width = acts.shape
    n_sections = lax.axis_size("pp")
    section = lax.axis_index("pp")
    rows = n_micro * per_group
    parts = SUBLANES // math.gcd(rows, SUBLANES)
    weights = (
        dense_gate[0],
        dense_up[0],
        dense_down[0],
        expert_gate[0, 0],
        expert_up[0, 0],
        expert_down[0, 0],
    )
    router_t = router[0].T

    fed = acts.swapaxes(0, 1)
    ids = route_ids[0].swapaxes(0, 1)
    n_groups = lax.axis_size("ep")
    tall = parts * rows

    def first(given):
        folded, flat, blank = layer(given, ids, None, norm_gain, router_t, weights, parts)
        return folded, flat, jnp.zeros((tall, LANES), jnp.bfloat16), blank

    def idle(given):
        folded = jnp.zeros((tall, width // parts), jnp.bfloat16)
        return folded, jnp.zeros((per_group, n_micro, width), jnp.bfloat16), *early_tags(ids, parts)

    folded, flat, *known = lax.cond(section == 0, first, idle, fed)
    for phase in range(1, n_sections):
        fed = lax.ppermute(folded, "pp", [(phase - 1, phase)])
        folded, flat = lax.cond(
            section == phase,
            lambda held, given: layer(given, ids, known, norm_gain, router_t, weights, parts)[:2],
            lambda held, given: held,
            (folded, flat),
            fed,
        )
    return flat.swapaxes(0, 1)[None]


def solution(mesh):
    return jax.shard_map(
        on_device,
        mesh=mesh,
        in_specs=(
            P(None, "ep", None),
            P("pp", None, "ep", None),
            P("pp", None),
            P("pp", None, None),
            P("pp", None, ("ep", "tp")),
            P("pp", None, ("ep", "tp")),
            P("pp", ("ep", "tp"), None),
            P("pp", "ep", None, "tp"),
            P("pp", "ep", None, "tp"),
            P("pp", "ep", "tp", None),
        ),
        out_specs=P("pp", None, "ep", None),
        check_vma=False,
    )
```

```python
import math

import jax
import jax.numpy as jnp
from jax import lax
from jax.experimental import pallas as pl
from jax.experimental.pallas import tpu as pltpu
from jax.sharding import PartitionSpec as P

LANES = 128
SUBLANES = 8
MIB = 1 << 20
FLIGHT = 12 * MIB
PIECE = 3 * MIB // 4
HIDDEN = 256
OUT = 512
WHOLE = pl.BlockSpec(memory_space=pltpu.VMEM)
SCALAR = pl.BlockSpec(memory_space=pltpu.SMEM)
OUTSIDE = pl.BlockSpec(memory_space=pl.ANY)


def exchange(blocks, axes):
    return lax.all_to_all(blocks, axes, split_axis=0, concat_axis=0, tiled=True)


def unfold(folded, parts):
    tall = folded.shape[0]
    lines = []
    for at, _, height in regions(tall // parts, parts):
        pieces = [folded[at + p * height : at + (p + 1) * height] for p in range(parts)]
        lines.append(jnp.concatenate(pieces, axis=1))
    return jnp.concatenate(lines, axis=0)


def sigmoid(v):
    return 1.0 / (1.0 + jnp.exp(-v))


def across(a, b):
    return lax.dot_general(a, b, (((1,), (1,)), ((), ())), preferred_element_type=jnp.float32)


def spread_of(pieces):
    count = sum(v.shape[1] for v in pieces)
    return sum(jnp.sum(v * v, axis=-1, keepdims=True) for v in pieces) / count


def regions(rows, parts):
    even = rows // SUBLANES * SUBLANES
    found = [(0, 0, even), (parts * even, even, rows - even)]
    return [region for region in found if region[2] > 0]


def place_in_block(rows, parts, part, row):
    for at, first, height in regions(rows, parts):
        if first <= row < first + height:
            return at + part * height + row - first


def pair_shapes(width, count):
    if count % LANES == 0:
        return [(width, 2 * count), (SUBLANES, LANES)]
    return [(width, count)] * 2


def refs_joined(held, source):
    return held.shape[1] == 2 * source.shape[1]


def column_cuts(total, size):
    return [(at, min(size, total - at)) for at in range(0, total, size)]


def write_tags(ids_ref, rows, parts, tags_ref):
    per_group, n_micro, top_count = ids_ref.shape
    step = math.gcd(n_micro, SUBLANES)
    tags_ref[...] = jnp.full(tags_ref.shape, -1.0, jnp.float32)
    for i in range(per_group):
        ids = ids_ref[i].astype(jnp.float32)
        for m in range(0, n_micro, step):
            at = place_in_block(rows, parts, 0, i * n_micro + m)
            tags_ref[at : at + step, :top_count] = ids[m : m + step]


def tags_kernel(parts, ids_ref, sent_ref, kept_ref, tags_ref):
    write_tags(ids_ref, tags_ref.shape[0] // parts, parts, tags_ref)
    block = tags_ref[...].astype(jnp.bfloat16)
    kept_ref[...] = block
    for g in range(sent_ref.shape[0]):
        sent_ref[g] = block


def settle_kernel(tags_ref, out_ref, sem):
    copy = pltpu.make_async_copy(tags_ref, out_ref, sem)
    copy.start()
    copy.wait()


def first_pack_kernel(parts, x_hbm, ids_hbm, sent_ref, kept_ref, kept_tags_ref, x_ref, ids_ref, tags_ref, block_ref, sems):
    copies = [
        pltpu.make_async_copy(x_hbm, x_ref, sems.at[0]),
        pltpu.make_async_copy(ids_hbm, ids_ref, sems.at[1]),
    ]
    for copy in copies:
        copy.start()
    for copy in copies:
        copy.wait()
    per_group, n_micro, _ = x_ref.shape
    rows, span = per_group * n_micro, block_ref.shape[1]
    step = math.gcd(n_micro, SUBLANES)
    write_tags(ids_ref, rows, parts, tags_ref)
    for i in range(per_group):
        mine = x_ref[i].astype(jnp.float32)
        for m in range(0, n_micro, step):
            for p in range(parts):
                at = place_in_block(rows, parts, p, i * n_micro + m)
                block_ref[at : at + step, :] = mine[m : m + step, p * span : (p + 1) * span]
    block, tags = block_ref[...].astype(jnp.bfloat16), tags_ref[...].astype(jnp.bfloat16)
    kept_ref[...] = block
    kept_tags_ref[...] = tags
    for g in range(sent_ref.shape[0]):
        sent_ref[g, :, :span] = block
        sent_ref[g, :, span:] = tags


def later_pack_kernel(x_ref, sent_ref):
    for g in range(sent_ref.shape[0]):
        sent_ref[g] = x_ref[...]


def base_kernel(n_real, top_count, parts, kept_ref, tags_ref, gain_ref, router_ref, base_ref, blank_ref):
    blank_ref[...] = jnp.zeros(blank_ref.shape, blank_ref.dtype)
    span = base_ref.shape[1]
    gains = [gain_ref[:, p * span : (p + 1) * span].astype(jnp.float32) for p in range(parts)]
    block, tags = kept_ref[...].astype(jnp.float32), tags_ref[...].astype(jnp.float32)
    for at, _, height in regions(base_ref.shape[0] // parts, parts):
        pieces = [block[at + p * height : at + (p + 1) * height] for p in range(parts)]
        ids = tags[at : at + height]
        scale = lax.rsqrt(spread_of(pieces) + 1e-06)
        normed = [(v * scale * gain).astype(jnp.bfloat16) for v, gain in zip(pieces, gains)]
        logits = sum(across(v, router_ref[:, p * span : (p + 1) * span]) for p, v in enumerate(normed))
        gates = sigmoid(logits)
        id_range = lax.broadcasted_iota(jnp.int32, gates.shape, 1)
        named = id_range.astype(jnp.float32)
        picked = sum((ids[:, k : k + 1] == named).astype(jnp.float32) for k in range(top_count))
        share = jnp.sum(jnp.where(id_range >= n_real, picked * gates, 0.0), axis=-1, keepdims=True)
        for p in range(parts):
            rows = slice(at + p * height, at + (p + 1) * height)
            base_ref[rows, :] = pieces[p] + share * normed[p].astype(jnp.float32)


def head_kernel(gate_ref, up_ref, head_ref, sems):
    size = head_ref.shape[1] // 2
    cols = pl.ds(gate_ref.shape[1] - size, size)
    copies = [
        pltpu.make_async_copy(source.at[:, cols], head_ref.at[:, pl.ds(i * size, size)], sems.at[i])
        for i, source in enumerate((gate_ref, up_ref))
    ]
    for copy in copies:
        copy.start()
    for copy in copies:
        copy.wait()


def layer_kernel(rows, parts, tagged, headed, place_ref, all_ref, gain_ref, router_ref, *refs):
    tags_ref, head_ref = None, None
    if not tagged:
        tags_ref, *refs = refs
    if headed:
        head_ref, *refs = refs
    early = head_ref.shape[1] // 2 if headed else 0
    sources, out_ref = refs[:6], refs[6]
    held = refs[7:13]
    d_down, e_down = held[2], held[5]
    normed_ref, coef_ref, d_hidden, e_hidden, value_ref, stage_ref, sems, out_sems = refs[13:]
    n_groups = all_ref.shape[0]
    span = out_ref.shape[2]
    width = parts * span
    place = place_ref[0]
    unit = 16 // math.gcd(rows, 16)
    unit = unit if n_groups % unit == 0 else n_groups

    out_cuts = column_cuts(span, OUT)
    if span % OUT == 0 and OUT % (2 * LANES) == 0:
        out_cuts = out_cuts[:-1] + [(span - OUT, OUT // 2), (span - OUT // 2, OUT // 2)]
    plan = []
    for which, hidden_ref in ((0, d_hidden), (3, e_hidden)):
        joined = hidden_ref.shape[1] % LANES == 0
        streamed = hidden_ref.shape[1] - (early if which == 0 else 0)
        for at, size in column_cuts(streamed, HIDDEN):
            spots = (2 * at, 2 * at + size) if joined else (at, at)
            plan += [(which, at, spots[0], size), (which + 1, at, spots[1], size)]
    for at, size in out_cuts:
        plan += [(which, p * span + at, p * span + at, size) for p in range(parts) for which in (2, 5)]
    held = tuple(
        held[i - 1] if i in (1, 4) and refs_joined(held[i - 1], sources[i]) else h for i, h in enumerate(held)
    )
    order, owned, volume, total = [], {}, [], 0
    for which, at, put, size in plan:
        height = held[which].shape[0]
        pieces = max(1, height * size * 2 // PIECE)
        pieces = pieces if height % pieces == 0 and height // pieces % 16 == 0 else 1
        owned[which, at] = range(len(order), len(order) + pieces)
        for k in range(pieces):
            lines = pl.ds(k * (height // pieces), height // pieces)
            source, target = sources[which].at[lines, pl.ds(at, size)], held[which].at[lines, pl.ds(put, size)]
            order.append(pltpu.make_async_copy(source, target, sems.at[len(order)]))
            total += height // pieces * size * 2
            volume.append(total)
    begun = [0]

    def start_until(limit):
        while begun[0] < len(order) and volume[begun[0]] <= limit:
            order[begun[0]].start()
            begun[0] += 1

    start_until(max(FLIGHT, volume[0]))

    def arrive(which, at):
        for i in owned[which, at]:
            order[i].wait()
            start_until(volume[i] + FLIGHT)

    def load(step, carry):
        blocks = [all_ref[step * unit + u].astype(jnp.float32) for u in range(unit)]
        if tags_ref is None:
            tags = [b[:, span:] for b in blocks]
        else:
            tags = [tags_ref[step * unit + u].astype(jnp.float32) for u in range(unit)]
        for at, first, height in regions(rows, parts):
            start = pl.multiple_of(n_groups * first + step * unit * height, 16)
            here = pl.ds(start, unit * height)
            pieces = [
                jnp.concatenate([b[at + p * height : at + (p + 1) * height, :span] for b in blocks], axis=0)
                for p in range(parts)
            ]
            ids = jnp.concatenate([t[at : at + height] for t in tags], axis=0)
            named = jnp.sum((ids == place.astype(jnp.float32)).astype(jnp.float32), axis=-1, keepdims=True)
            scale = lax.rsqrt(spread_of(pieces) + 1e-06)
            for p, v in enumerate(pieces):
                gain = gain_ref[:, p * span : (p + 1) * span].astype(jnp.float32)
                normed_ref[here, p * span : (p + 1) * span] = (v * scale * gain).astype(jnp.bfloat16)
            coef_ref[here, :] = jnp.broadcast_to(named, (unit * height, LANES))
        return carry

    lax.fori_loop(0, n_groups // unit, load, 0)

    logits = across(normed_ref[...], router_ref[...])
    mine = lax.broadcasted_iota(jnp.int32, logits.shape, 1) == place
    gate = jnp.sum(jnp.where(mine, sigmoid(logits), 0.0), axis=-1, keepdims=True)
    coef_ref[...] = coef_ref[...] * gate

    def hidden(which, target):
        joined = target.shape[1] % LANES == 0
        streamed = target.shape[1]
        if which == 0 and headed:
            streamed -= early
            pair = jnp.dot(normed_ref[...], head_ref[...], preferred_element_type=jnp.float32)
            gate_part, up_part = pair[:, :early], pair[:, early:]
            target[:, streamed:] = (gate_part * sigmoid(gate_part) * up_part).astype(jnp.bfloat16)
        for at, size in column_cuts(streamed, HIDDEN):
            arrive(which, at)
            arrive(which + 1, at)
            if joined:
                pair = jnp.dot(
                    normed_ref[...], held[which][:, 2 * at : 2 * (at + size)], preferred_element_type=jnp.float32
                )
                gate_part, up_part = pair[:, :size], pair[:, size:]
            else:
                gate_part, up_part = (
                    jnp.dot(normed_ref[...], held[w][:, at : at + size], preferred_element_type=jnp.float32)
                    for w in (which, which + 1)
                )
            target[:, at : at + size] = (gate_part * sigmoid(gate_part) * up_part).astype(jnp.bfloat16)

    hidden(0, d_hidden)
    hidden(3, e_hidden)

    leaving = []
    for at, size in out_cuts:
        for which in (2, 5):
            for p in range(parts):
                arrive(which, p * span + at)
        for p in range(parts):
            cols = slice(p * span + at, p * span + at + size)
            dense = jnp.dot(d_hidden[...], d_down[:, cols], preferred_element_type=jnp.float32)
            routed = jnp.dot(e_hidden[...], e_down[:, cols], preferred_element_type=jnp.float32)
            value_ref[:, p * OUT : p * OUT + size] = dense + coef_ref[:, :1] * routed

        def pack(step, carry):
            rows_of = []
            for _, first, height in regions(rows, parts):
                start = pl.multiple_of(n_groups * first + step * unit * height, SUBLANES)
                rows_of.append((height, value_ref[pl.ds(start, unit * height), :]))
            for u in range(unit):
                pieces = [
                    tall[u * height : (u + 1) * height, p * OUT : p * OUT + size]
                    for height, tall in rows_of
                    for p in range(parts)
                ]
                block = jnp.concatenate(pieces, axis=0).astype(out_ref.dtype)
                stage_ref[step * unit + u, :, at : at + size] = block
            return carry

        lax.fori_loop(0, n_groups // unit, pack, 0)
        cols = pl.ds(at, size)
        leaving.append(pltpu.make_async_copy(stage_ref.at[:, :, cols], out_ref.at[:, :, cols], out_sems.at[len(leaving)]))
        leaving[-1].start()
    for copy in leaving:
        copy.wait()


def combine_kernel(parts, got_ref, base_ref, folded_ref, flat_ref, total_ref):
    per_group, n_micro, width = flat_ref.shape
    rows, span = n_micro * per_group, base_ref.shape[1]
    total = base_ref[...]
    for g in range(got_ref.shape[0]):
        total = total + got_ref[g].astype(jnp.float32)
    folded_ref[...] = total.astype(jnp.bfloat16)
    total_ref[...] = total
    step = math.gcd(n_micro, SUBLANES)
    for i in range(per_group):
        for m in range(0, n_micro, step):
            for p in range(parts):
                at = place_in_block(rows, parts, p, i * n_micro + m)
                cols = slice(p * span, (p + 1) * span)
                flat_ref[i, m : m + step, cols] = total_ref[at : at + step, :].astype(jnp.bfloat16)


def layer(fed, ids, known, gain, router_t, weights, parts):
    per_group, n_micro, top_count = ids.shape
    n_groups = lax.axis_size("ep")
    n_pairs = lax.axis_size("tp")
    place = lax.axis_index("ep")
    width = gain.shape[1]
    rows, span = n_micro * per_group, width // parts
    tall, wide = parts * rows, span + LANES
    count = n_groups * rows

    params = pltpu.CompilerParams(vmem_limit_bytes=16 * MIB)
    if known is None:
        sent, kept, tags = pl.pallas_call(
            lambda *refs: first_pack_kernel(parts, *refs),
            out_shape=[
                jax.ShapeDtypeStruct((n_groups, tall, wide), jnp.bfloat16),
                jax.ShapeDtypeStruct((tall, span), jnp.bfloat16),
                jax.ShapeDtypeStruct((tall, LANES), jnp.bfloat16),
            ],
            in_specs=[OUTSIDE, OUTSIDE],
            out_specs=[WHOLE] * 3,
            scratch_shapes=[
                pltpu.VMEM(fed.shape, fed.dtype),
                pltpu.VMEM(ids.shape, ids.dtype),
                pltpu.VMEM((tall, LANES), jnp.float32),
                pltpu.VMEM((tall, span), jnp.float32),
                pltpu.SemaphoreType.DMA((2,)),
            ],
            compiler_params=params,
            name="pack",
        )(fed, ids)
        all_tags = []
    else:
        kept, tags, all_tags = fed, known[0], [known[1]]
        sent = pl.pallas_call(
            later_pack_kernel,
            out_shape=jax.ShapeDtypeStruct((n_groups, tall, span), jnp.bfloat16),
            in_specs=[WHOLE],
            out_specs=WHOLE,
            compiler_params=params,
            name="pack",
        )(fed)
    gathered = exchange(sent, "ep")

    blank_groups = n_groups if known is None else 1
    base, blank = pl.pallas_call(
        lambda *refs: base_kernel(n_groups, top_count, parts, *refs),
        out_shape=[
            jax.ShapeDtypeStruct((tall, span), jnp.float32),
            jax.ShapeDtypeStruct((blank_groups, tall, LANES), jnp.bfloat16),
        ],
        in_specs=[WHOLE] * 4,
        out_specs=[WHOLE, WHOLE],
        compiler_params=pltpu.CompilerParams(vmem_limit_bytes=8 * MIB),
        cost_estimate=pl.CostEstimate(flops=int(1e8), bytes_accessed=int(1e6), transcendentals=0),
        name="base",
    )(kept, tags, gain, router_t)

    n_dense, n_expert = weights[0].shape[1], weights[3].shape[1]
    early = n_dense % HIDDEN if n_dense > HIDDEN and n_dense % LANES == 0 else 0
    heads = []
    if early:
        head = pl.pallas_call(
            head_kernel,
            out_shape=pltpu.VMEM((width, 2 * early), jnp.bfloat16),
            in_specs=[pl.BlockSpec(memory_space=pltpu.HBM)] * 2,
            out_specs=WHOLE,
            scratch_shapes=[pltpu.SemaphoreType.DMA((2,))],
            compiler_params=pltpu.CompilerParams(vmem_limit_bytes=4 * MIB),
            cost_estimate=pl.CostEstimate(flops=int(1e9), bytes_accessed=early * width * 4, transcendentals=0),
            name="head",
        )(*(pltpu.with_memory_space_constraint(w, pltpu.HBM) for w in weights[:2]))
        heads = [pltpu.with_memory_space_constraint(head, pltpu.VMEM)]
    weights = [pltpu.with_memory_space_constraint(w, pltpu.HBM) for w in weights]
    partial = pl.pallas_call(
        lambda *refs: layer_kernel(rows, parts, known is None, early > 0, *refs),
        out_shape=pltpu.HBM((n_groups, tall, span), jnp.bfloat16),
        in_specs=[SCALAR] + [WHOLE] * (3 + len(all_tags) + len(heads)) + [pl.BlockSpec(memory_space=pltpu.HBM)] * 6,
        out_specs=pl.BlockSpec(memory_space=pltpu.HBM),
        scratch_shapes=[
            *(pltpu.VMEM(shape, jnp.bfloat16) for shape in pair_shapes(width, n_dense)),
            pltpu.VMEM((n_dense, width), jnp.bfloat16),
            *(pltpu.VMEM(shape, jnp.bfloat16) for shape in pair_shapes(width, n_expert)),
            pltpu.VMEM((n_expert, width), jnp.bfloat16),
            pltpu.VMEM((count, width), jnp.bfloat16),
            pltpu.VMEM((count, LANES), jnp.float32),
            pltpu.VMEM((count, n_dense), jnp.bfloat16),
            pltpu.VMEM((count, n_expert), jnp.bfloat16),
            pltpu.VMEM((count, parts * OUT), jnp.float32),
            pltpu.VMEM((n_groups, tall, span), jnp.bfloat16),
            pltpu.SemaphoreType.DMA((128,)),
            pltpu.SemaphoreType.DMA((16,)),
        ],
        compiler_params=pltpu.CompilerParams(vmem_limit_bytes=50 * MIB),
        cost_estimate=pl.CostEstimate(
            flops=6 * count * width * (n_dense + n_expert),
            bytes_accessed=6 * width * (n_dense + n_expert),
            transcendentals=0,
        ),
        name="layer",
    )(place.reshape(1).astype(jnp.int32), gathered, gain, router_t, *all_tags, *heads, *weights)

    share = tall // n_pairs
    received = exchange(partial.reshape(n_groups * n_pairs, share, span), ("ep", "tp"))
    if n_pairs > 1:
        kept_base = lax.dynamic_slice_in_dim(base, lax.axis_index("tp") * share, share, 0)
        part = (kept_base + jnp.sum(received.astype(jnp.float32), axis=0)).astype(jnp.bfloat16)
        folded = lax.all_gather(part, "tp", axis=0, tiled=True)
        return folded, unfold(folded, parts).reshape(per_group, n_micro, width), blank
    folded, flat = pl.pallas_call(
        lambda *refs: combine_kernel(parts, *refs),
        out_shape=[
            jax.ShapeDtypeStruct((tall, span), jnp.bfloat16),
            jax.ShapeDtypeStruct((per_group, n_micro, width), jnp.bfloat16),
        ],
        in_specs=[WHOLE, WHOLE],
        out_specs=[WHOLE, WHOLE],
        scratch_shapes=[pltpu.VMEM((tall, span), jnp.float32)],
        compiler_params=pltpu.CompilerParams(vmem_limit_bytes=8 * MIB),
        name="combine",
    )(received, base)
    return folded, flat, blank


def early_tags(ids, parts):
    per_group, n_micro, _ = ids.shape
    n_groups, tall = lax.axis_size("ep"), parts * per_group * n_micro
    sent, tags = pl.pallas_call(
        lambda *refs: tags_kernel(parts, *refs),
        out_shape=[
            jax.ShapeDtypeStruct((n_groups, tall, LANES), jnp.bfloat16),
            jax.ShapeDtypeStruct((tall, LANES), jnp.bfloat16),
        ],
        in_specs=[WHOLE],
        out_specs=[WHOLE, WHOLE],
        scratch_shapes=[pltpu.VMEM((tall, LANES), jnp.float32)],
        compiler_params=pltpu.CompilerParams(vmem_limit_bytes=8 * MIB),
        name="tags",
    )(ids)
    settled = pl.pallas_call(
        settle_kernel,
        out_shape=pltpu.HBM(sent.shape, sent.dtype),
        in_specs=[WHOLE],
        out_specs=pl.BlockSpec(memory_space=pltpu.HBM),
        scratch_shapes=[pltpu.SemaphoreType.DMA],
        compiler_params=pltpu.CompilerParams(vmem_limit_bytes=8 * MIB),
        name="settle",
    )(exchange(sent, "ep"))
    return tags, settled


def on_device(
    acts,
    route_ids,
    norm_gain,
    router,
    dense_gate,
    dense_up,
    dense_down,
    expert_gate,
    expert_up,
    expert_down,
):
    n_micro, per_group, width = acts.shape
    n_sections = lax.axis_size("pp")
    section = lax.axis_index("pp")
    rows = n_micro * per_group
    parts = SUBLANES // math.gcd(rows, SUBLANES)
    weights = (
        dense_gate[0],
        dense_up[0],
        dense_down[0],
        expert_gate[0, 0],
        expert_up[0, 0],
        expert_down[0, 0],
    )
    router_t = router[0].T

    fed = acts.swapaxes(0, 1)
    ids = route_ids[0].swapaxes(0, 1)
    n_groups = lax.axis_size("ep")
    tall = parts * rows

    def first(given):
        folded, flat, blank = layer(given, ids, None, norm_gain, router_t, weights, parts)
        return folded, flat, jnp.zeros((tall, LANES), jnp.bfloat16), blank

    def idle(given):
        folded = jnp.zeros((tall, width // parts), jnp.bfloat16)
        return folded, jnp.zeros((per_group, n_micro, width), jnp.bfloat16), *early_tags(ids, parts)

    folded, flat, *known = lax.cond(section == 0, first, idle, fed)
    for phase in range(1, n_sections):
        fed = lax.ppermute(folded, "pp", [(phase - 1, phase)])
        folded, flat = lax.cond(
            section == phase,
            lambda held, given: layer(given, ids, known, norm_gain, router_t, weights, parts)[:2],
            lambda held, given: held,
            (folded, flat),
            fed,
        )
    return flat.swapaxes(0, 1)[None]


def solution(mesh):
    return jax.shard_map(
        on_device,
        mesh=mesh,
        in_specs=(
            P(None, "ep", None),
            P("pp", None, "ep", None),
            P("pp", None),
            P("pp", None, None),
            P("pp", None, ("ep", "tp")),
            P("pp", None, ("ep", "tp")),
            P("pp", ("ep", "tp"), None),
            P("pp", "ep", None, "tp"),
            P("pp", "ep", None, "tp"),
            P("pp", "ep", "tp", None),
        ),
        out_specs=P("pp", None, "ep", None),
        check_vma=False,
    )
```
